128 devices in a mesh: section: 32 (over y, z, core), tensor: 4 (over x).
Axes of the slice: x: 4, y: 4, z: 4, core: 2. Of those that a mesh axis runs over, the one named last changes fastest.
Arguments:
- section_input: bfloat16 [32, 512, 4096], P('section', 'tensor'), may hold values from -6 to 6
- history: bfloat16 [32, 7, 512, 4096], P('section', None, 'tensor'), may hold values from -6 to 6
- query_weight: bfloat16 [32, 4096, 3072], P('section', None, 'tensor'), may hold values from -0.4 to 0.4
- key_weight: bfloat16 [32, 4096, 512], P('section', None, 'tensor'), may hold values from -0.4 to 0.4
- value_weight: bfloat16 [32, 4096, 512], P('section', None, 'tensor'), may hold values from -0.09375 to 0.09375
- output_weight: bfloat16 [32, 3072, 4096], P('section', 'tensor'), may hold values from -0.5 to 0.5
- mix_weights: float32 [32, 8], replicated, may hold values from 0.2 to 0.6
Outputs:
- next_input: bfloat16 [32, 512, 4096], P('section', 'tensor')
The draws below stay inside these ranges and needn't reach their ends.
All inputs are finite; a program needn't handle non-finite values.
Results may differ from the reference program's by a relative error of at most 0.013.
The reference program's roundings to bfloat16 on the way count: a program that leaves them out, or rounds other values in their place, can miss the bound.
Values may be sent and summed in bfloat16 or wider, within the bound.
A program may use at most 128 MiB of HBM per device.

```python
import math
import jax
import jax.numpy as jnp
from jax import lax

D = 4096
HEADS = 48
KV_HEADS = 8
HEAD_DIM = 64
DILATION_STRIDE = 4
SEQ = 512
HIST = 7
N_SECTION = 32
N_TENSOR = 4


def draw_query_weight(key, part):
    entries = jax.random.normal(jax.random.fold_in(key, 11), (N_SECTION, D, HEADS * HEAD_DIM), jnp.float32) / jnp.sqrt(jnp.float32(D))
    return jnp.clip(entries, -0.39, 0.39).astype(jnp.bfloat16)


def draw_key_weight(key, part):
    entries = jax.random.normal(jax.random.fold_in(key, 13), (N_SECTION, D, KV_HEADS * HEAD_DIM), jnp.float32) / jnp.sqrt(jnp.float32(D))
    return jnp.clip(entries, -0.39, 0.39).astype(jnp.bfloat16)


def steps_of(rng, extent, shards, low, high):
    level, own = 1.0, jax.random.fold_in(rng, 6)
    for dim, shards_of in shards:
        heights = jnp.exp(jax.random.uniform(jax.random.fold_in(own, dim), (shards_of,), jnp.float32, low / len(shards), high / len(shards)))
        level = level * jnp.repeat(heights, extent[dim] // shards_of).reshape([-1 if axis == dim else 1 for axis in range(len(extent))])
    return level


def noise(key, shape, spread, reach, shards=(), kind=jnp.bfloat16):
    factor_of = steps_of(key, shape, shards, -0.22, 0.18) if shards else 1.0
    result = jax.random.normal(key, shape, jnp.float32) * spread * factor_of
    return jnp.minimum(jnp.maximum(result, -reach), reach).astype(kind)


def setup_inputs(seed: int = 0) -> dict:
    seeds = jax.random.split(jax.random.key(seed), 8)
    return {
        "section_input": noise(seeds[0], (N_SECTION, SEQ, D), 1.0, 6.0, ((0, 32), (1, 4))),
        "history": noise(seeds[1], (N_SECTION, HIST, SEQ, D), 1.0, 6.0, ((0, 32), (2, 4))),
        "query_weight": draw_query_weight(jax.random.fold_in(seeds[7], 71), 0),
        "key_weight": draw_key_weight(jax.random.fold_in(seeds[7], 71), 0),
        "value_weight": noise(seeds[4], (N_SECTION, D, KV_HEADS * HEAD_DIM), D ** -0.5, 0.09375, ((0, 32), (2, 4))),
        "output_weight": noise(seeds[5], (N_SECTION, HEADS * HEAD_DIM, D), 0.08, 0.5, ((0, 32), (1, 4))),
        "mix_weights": jnp.clip(jax.random.uniform(seeds[6], (N_SECTION, HIST + 1), jnp.float32, 0.2, 0.6), 0.2, 0.6),
    }


def normalize(token_rows):
    values = token_rows.astype(jnp.float32)
    inv_scale = lax.rsqrt(lax.optimization_barrier(jnp.mean(values * values, axis=-1, keepdims=True)) + 1e-05)
    return (values * inv_scale).astype(jnp.bfloat16)

def one_section(operands):
    token_rows, query_part, key_part, value_part, output_part = operands
    seq_len = token_rows.shape[0]
    normed = normalize(token_rows)
    query_rows = jnp.dot(normed, query_part, preferred_element_type=jnp.float32).astype(jnp.bfloat16)
    key_rows = jnp.dot(normed, key_part, preferred_element_type=jnp.float32).astype(jnp.bfloat16)
    value_rows = jnp.dot(normed, value_part, preferred_element_type=jnp.float32).astype(jnp.bfloat16)
    per_group = HEADS // KV_HEADS
    query_heads = query_rows.astype(jnp.float32).reshape(seq_len, KV_HEADS, per_group, HEAD_DIM)
    key_heads = key_rows.astype(jnp.float32).reshape(seq_len, KV_HEADS, HEAD_DIM)
    value_heads = value_rows.astype(jnp.float32).reshape(seq_len, KV_HEADS, HEAD_DIM)
    scores = jnp.einsum('tgjd,sgd->gjts', query_heads, key_heads) / math.sqrt(HEAD_DIM)
    positions = jnp.arange(seq_len, dtype=jnp.int32)
    scores = jnp.where(positions[:, None] >= positions[None, :], scores, -1e+30)
    softmax_weights = jax.nn.softmax(scores, axis=-1).astype(jnp.bfloat16)
    heads_out = jnp.einsum('gjts,sgd->tgjd', softmax_weights.astype(jnp.float32), value_heads)
    heads_out = heads_out.astype(jnp.bfloat16).reshape(seq_len, HEADS * HEAD_DIM)
    grouped = heads_out.astype(jnp.float32).reshape(seq_len, N_TENSOR, -1)
    grouped_weight = output_part.astype(jnp.float32).reshape(N_TENSOR, -1, D)
    partials = jnp.einsum('tnc,ncd->ntd', grouped, grouped_weight)
    partials = lax.optimization_barrier(partials.astype(jnp.bfloat16)).astype(jnp.float32)
    attention_sum = lax.optimization_barrier(jnp.sum(partials, axis=0))
    return (token_rows.astype(jnp.float32) + attention_sum).astype(jnp.bfloat16)

def reference(section_input, history, query_weight, key_weight, value_weight, output_weight, mix_weights):
    block_outs = lax.map(one_section, (section_input, query_weight, key_weight, value_weight, output_weight))
    section_numbers = jnp.arange(N_SECTION, dtype=jnp.int32)
    mixed_sum = mix_weights[:, 0][:, None, None] * block_outs.astype(jnp.float32)
    for history_slot in range(1, HIST + 1):
        sender_section = section_numbers - DILATION_STRIDE * history_slot
        picked = jnp.take(history[:, history_slot - 1], jnp.maximum(sender_section, 0).astype(jnp.int32), axis=0)
        factor = jnp.where(sender_section >= 0, mix_weights[:, history_slot], jnp.float32(0.0))
        mixed_sum = mixed_sum + factor[:, None, None] * picked.astype(jnp.float32)
    mixed = mixed_sum.astype(jnp.bfloat16)
    return jnp.concatenate([mixed[-1:], mixed[:-1]], axis=0)
```

```python
import math

import jax
import jax.numpy as jnp
from jax import lax
from jax.experimental import pallas as pl
from jax.experimental.pallas import tpu as pltpu
from jax.sharding import PartitionSpec as P

HEAD_DIM = 64
MESH = pl.DeviceIdType.MESH
F32 = jnp.float32
BF16 = jnp.bfloat16
ROWS = 128
HALF = 64
SUB = 16
SUBS = HALF // SUB
D = 4096
SEQ = 512
QW = 768
PAIRS = QW // 128
AG = 0
YS = 6
ZS = 18
XS = 20
XT = 24
FS = XT + 2 * SUBS
N_COPIES = FS + 2 * SUBS
N_LOADS = 11


def rows_at(start, size, step):
    return pl.ds(pl.multiple_of(start, step), size)


def whole_tick(
    x_hbm, hist_hbm, wq_hbm, wk_hbm, wv_hbm, wo_hbm, mix, out_hbm,
    xv, xg, wqkv, wo, qkv, kc, vc, heads, part, xbuf, xtail, ybuf, ystage, hA, hB, h1, zs, zr, hs, stage,
    send_sem, recv_sem, load_sem,
):
    s = lax.axis_index("section")
    x = lax.axis_index("tensor")
    y = s // 8
    zc = lax.rem(s // 4, 2)
    x_right, x_left, x_opp = lax.rem(x + 1, 4), lax.rem(x + 3, 4), lax.rem(x + 2, 4)
    y_right, y_left = lax.rem(y + 1, 4), lax.rem(y + 3, 4)
    s_right, s_left = lax.rem(s + 8, 32), lax.rem(s + 24, 32)
    s_pair = s + 4 - 8 * zc
    s_next, s_prev = lax.rem(s + 1, 32), lax.rem(s + 31, 32)
    right, left = (s, x_right), (s, x_left)
    up, down = (s_right, x), (s_left, x)
    pair, following, preceding = (s_pair, x), (s_next, x), (s_prev, x)

    barrier = pltpu.get_barrier_semaphore()
    for other in (right, left, up, down, pair, following, preceding):
        pl.semaphore_signal(barrier, inc=1, device_id=other, device_id_type=MESH)

    def load(number, src, dst):
        copy = pltpu.make_async_copy(src, dst, load_sem.at[number])
        copy.start()
        return copy

    other_c = 1 - zc
    columns = (other_c, zc)
    top, bottom = pl.ds(0, HALF), pl.ds(HALF, HALF)

    def slot(dy, c):
        return 2 * dy + c - zc - 1

    load_x = load(0, x_hbm, xv)
    load_w = [
        load(1, wq_hbm, wqkv.at[:, pl.ds(0, QW)]),
        load(2, wk_hbm, wqkv.at[:, pl.ds(QW, 128)]),
        load(3, wv_hbm, wqkv.at[:, pl.ds(QW + 128, 128)]),
    ]
    load_h = []
    for i, c in enumerate(columns):
        load_h.append(
            (
                load(4 + 2 * i, hist_hbm.at[slot(3, c), top], hA.at[i]),
                load(5 + 2 * i, hist_hbm.at[slot(1, c), bottom], hB.at[i]),
            )
        )
    load_h1 = load(8, hist_hbm.at[0], h1)
    load_wo = load(9, wo_hbm, wo)

    def send(number, src, dst, device):
        copy = pltpu.make_async_remote_copy(
            src_ref=src,
            dst_ref=dst,
            send_sem=send_sem.at[number],
            recv_sem=recv_sem.at[number],
            device_id=device,
            device_id_type=MESH,
        )
        copy.start()
        copies[number] = copy

    copies = {}

    load_x.wait()

    def normalize_rows(i, carry):
        r = rows_at(i * 16, 16, 16)
        values = xv[r, :].astype(F32)
        inv = lax.rsqrt(jnp.mean(values * values, axis=-1, keepdims=True) + 1e-05)
        xg[x, r, :] = (values * inv).astype(BF16)
        return carry

    lax.fori_loop(0, ROWS // 16, normalize_rows, 0)

    pl.semaphore_wait(barrier, 7)

    def own_rows(number, half, device):
        send(number, xg.at[x, half], xg.at[x, half], device)

    own_rows(AG + 0, top, right)
    own_rows(AG + 3, bottom, left)
    own_rows(AG + 1, bottom, right)
    own_rows(AG + 4, top, left)

    def raw_history(i):
        c = columns[i]
        n = YS + 6 * i
        send(n + 0, hist_hbm.at[slot(2, c), top], ybuf.at[i, 0], down)
        send(n + 1, hist_hbm.at[slot(2, c), bottom], ybuf.at[i, 1], up)
        send(n + 2, hist_hbm.at[slot(3, c), bottom], ybuf.at[i, 2], down)
        send(n + 3, hist_hbm.at[slot(1, c), top], ybuf.at[i, 3], up)

    raw_history(0)

    def weight(y_dst, c, y_src):
        k = 2 * (y_dst - y_src) + c - zc
        s_dst = y_dst * 8 + c * 4 + lax.rem(s, 4)
        return jnp.where(y_dst > y_src, mix[s_dst, jnp.clip(k, 0, 7)], F32(0.0))

    def pieces(count, body):
        def step(j, carry):
            body(j)
            return carry

        lax.fori_loop(0, count, step, 0)

    def project(b):
        r = rows_at(b * ROWS, ROWS, ROWS)

        def tile(j):
            cols = rows_at(j * 256, 256, 256)
            qkv[r, cols] = jnp.dot(xg[b], wqkv[:, cols], preferred_element_type=F32).astype(BF16)

        pieces(4, tile)
        low = lax.broadcasted_iota(jnp.int32, (ROWS, 128), 1) < HEAD_DIM
        r_hi = rows_at(b * ROWS + SEQ, ROWS, ROWS)
        for column, dst in ((QW, kc), (QW + 128, vc)):
            both = qkv[r, pl.ds(column, 128)].astype(F32)
            turned = pltpu.roll(both, HEAD_DIM, 1)
            zero = jnp.zeros_like(both)
            dst[0, r, :] = jnp.where(low, both, zero).astype(BF16)
            dst[0, r_hi, :] = jnp.where(low, zero, turned).astype(BF16)
            dst[1, r, :] = jnp.where(low, turned, zero).astype(BF16)
            dst[1, r_hi, :] = jnp.where(low, zero, both).astype(BF16)

    exponent_scale = math.log2(math.e) / math.sqrt(HEAD_DIM)

    def attend(b):
        r = rows_at(b * ROWS, ROWS, ROWS)
        row = lax.broadcasted_iota(jnp.int32, (ROWS, SEQ), 0) + b * ROWS
        seen = row >= lax.broadcasted_iota(jnp.int32, (ROWS, SEQ), 1)

        def two_heads(p):
            g = p // (PAIRS // 2)
            cols = rows_at(p * 128, 128, 128)
            scores = lax.dot_general(
                qkv[r, cols], kc[g], (((1,), (1,)), ((), ())), preferred_element_type=F32
            )
            out = []
            for h in range(2):
                own = jnp.where(seen, scores[:, h * SEQ : (h + 1) * SEQ], -1e30)
                high = jnp.max(own, axis=-1, keepdims=True)
                e = jnp.exp2((own - high) * exponent_scale)
                total = jnp.sum(e, axis=-1, keepdims=True)
                out.append((e * (1.0 / total)).astype(BF16))
            probs = jnp.concatenate(out, axis=1)
            heads[:, cols] = jnp.dot(probs, vc[g], preferred_element_type=F32).astype(BF16)

        pieces(PAIRS, two_heads)

        def tile(j):
            cols = rows_at(j * 512, 512, 512)
            part[b, :, cols] = jnp.dot(heads[...], wo[:, cols], preferred_element_type=F32).astype(BF16)

        pieces(D // 512, tile)

    for copy in load_w:
        copy.wait()
    project(x)

    copies[AG + 0].wait_recv()
    send(AG + 2, xg.at[x_left, top], xg.at[x_left, top], right)
    copies[AG + 3].wait_recv()
    send(AG + 5, xg.at[x_right, bottom], xg.at[x_right, bottom], left)

    def merge_history(i):
        c = columns[i]
        n = YS + 6 * i
        for copy in load_h[i]:
            copy.wait()
        copies[n + 0].wait_recv()
        theirs, mine = weight(y_left, c, y_right), weight(y_left, c, y)

        def down_rows(j):
            r = rows_at(j * 16, 16, 16)
            ystage[i, 0, r, :] = (
                theirs * ybuf[i, 0, r, :].astype(F32) + mine * hA[i, r, :].astype(F32)
            ).astype(BF16)

        pieces(HALF // 16, down_rows)
        send(n + 4, ystage.at[i, 0], ybuf.at[i, 4], down)
        copies[n + 1].wait_recv()
        theirs_up, mine_up = weight(y_right, c, y_left), weight(y_right, c, y)

        def up_rows(j):
            r = rows_at(j * 16, 16, 16)
            ystage[i, 1, r, :] = (
                theirs_up * ybuf[i, 1, r, :].astype(F32) + mine_up * hB[i, r, :].astype(F32)
            ).astype(BF16)

        pieces(HALF // 16, up_rows)
        send(n + 5, ystage.at[i, 1], ybuf.at[i, 5], up)

    merge_history(0)
    raw_history(1)

    copies[AG + 1].wait_recv()
    project(x_left)
    copies[AG + 4].wait_recv()
    project(x_right)
    copies[AG + 2].wait_recv()
    copies[AG + 5].wait_recv()
    project(x_opp)
    load_wo.wait()
    attend(x_opp)
    send(XS + 0, part.at[x_opp, top], xbuf.at[0], left)
    send(XS + 1, part.at[x_opp, bottom], xbuf.at[1], right)

    def column_sums(i):
        c = columns[i]
        n = YS + 6 * i
        for m in (2, 3, 4, 5):
            copies[n + m].wait_recv()
        below, above = weight(y, c, y_left), weight(y, c, y_right)

        def of(r):
            upper = below * ybuf[i, 3, r, :].astype(F32) + ybuf[i, 4, r, :].astype(F32)
            lower = ybuf[i, 5, r, :].astype(F32) + above * ybuf[i, 2, r, :].astype(F32)
            return upper, lower

        return of

    load_h1.wait()
    sums = column_sums(0)
    first = jnp.where(zc == 0, mix[jnp.minimum(s + 4, 31), 1], F32(0.0))

    def pair_rows(j):
        r = rows_at(j * 16, 16, 16)
        r_low = rows_at(j * 16 + HALF, 16, 16)
        upper, lower = sums(r)
        zs[r, :] = (upper + first * h1[r, :].astype(F32)).astype(BF16)
        zs[r_low, :] = (lower + first * h1[r_low, :].astype(F32)).astype(BF16)

    pieces(HALF // 16, pair_rows)
    send(ZS + 0, zs.at[top], zr.at[top], pair)
    send(ZS + 1, zs.at[bottom], zr.at[bottom], pair)

    attend(x_left)
    send(XS + 2, part.at[x_left, bottom], xbuf.at[2], left)
    attend(x_right)
    send(XS + 3, part.at[x_right, top], xbuf.at[3], right)
    attend(x)
    merge_history(1)

    copies[XS + 0].wait_recv()
    copies[XS + 1].wait_recv()
    for i in range(SUBS):
        r = pl.ds(i * SUB, SUB)
        part[x_left, r, :] = (part[x_left, r, :].astype(F32) + xbuf[0, r, :].astype(F32)).astype(BF16)
        send(XT + i, part.at[x_left, r], xtail.at[0, r], left)
        r_low = pl.ds(HALF + i * SUB, SUB)
        part[x_right, r_low, :] = (
            part[x_right, r_low, :].astype(F32) + xbuf[1, r, :].astype(F32)
        ).astype(BF16)
        send(XT + SUBS + i, part.at[x_right, r_low], xtail.at[1, r], right)

    own_sums = column_sums(1)
    copies[ZS + 0].wait_recv()
    copies[ZS + 1].wait_recv()

    def history_rows(j):
        r = rows_at(j * 16, 16, 16)
        r_low = rows_at(j * 16 + HALF, 16, 16)
        upper, lower = own_sums(r)
        hs[r, :] = upper + zr[r, :].astype(F32)
        hs[r_low, :] = lower + zr[r_low, :].astype(F32)

    pieces(HALF // 16, history_rows)

    copies[XS + 2].wait_recv()
    copies[XS + 3].wait_recv()
    own_weight = mix[s, 0]
    for i in range(SUBS):
        r = pl.ds(i * SUB, SUB)
        for side in range(2):
            rr = pl.ds(side * HALF + i * SUB, SUB)
            copies[XT + side * SUBS + i].wait_recv()

            def mix_columns(j):
                cols = rows_at(j * 1024, 1024, 1024)
                total = (
                    part[x, rr, cols].astype(F32)
                    + xtail[side, r, cols].astype(F32)
                    + xbuf[3 - side, r, cols].astype(F32)
                )
                block_out = (xv[rr, cols].astype(F32) + total).astype(BF16)
                stage[rr, cols] = (own_weight * block_out.astype(F32) + hs[rr, cols]).astype(BF16)

            pieces(D // 1024, mix_columns)
            send(FS + side * SUBS + i, stage.at[rr], out_hbm.at[rr], following)

    for number in range(N_COPIES):
        copies[number].wait_send()
    for number in range(FS, FS + 2 * SUBS):
        copies[number].wait_recv()


def on_device(section_input, history, query_weight, key_weight, value_weight, output_weight, mix_weights):
    anywhere = pl.BlockSpec(memory_space=pl.ANY)
    out = pl.pallas_call(
        whole_tick,
        out_shape=jax.ShapeDtypeStruct((ROWS, D), BF16),
        in_specs=[anywhere] * 6 + [pl.BlockSpec(memory_space=pltpu.SMEM)],
        out_specs=anywhere,
        scratch_shapes=[
            pltpu.VMEM((ROWS, D), BF16),
            pltpu.VMEM((4, ROWS, D), BF16),
            pltpu.VMEM((D, QW + 256), BF16),
            pltpu.VMEM((QW, D), BF16),
            pltpu.VMEM((SEQ, QW + 256), BF16),
            pltpu.VMEM((2, 2 * SEQ, 128), BF16),
            pltpu.VMEM((2, 2 * SEQ, 128), BF16),
            pltpu.VMEM((ROWS, QW), BF16),
            pltpu.VMEM((4, ROWS, D), BF16),
            pltpu.VMEM((4, HALF, D), BF16),
            pltpu.VMEM((2, HALF, D), BF16),
            pltpu.VMEM((2, 6, HALF, D), BF16),
            pltpu.VMEM((2, 2, HALF, D), BF16),
            pltpu.VMEM((2, HALF, D), BF16),
            pltpu.VMEM((2, HALF, D), BF16),
            pltpu.VMEM((ROWS, D), BF16),
            pltpu.VMEM((ROWS, D), BF16),
            pltpu.VMEM((ROWS, D), BF16),
            pltpu.VMEM((ROWS, D), F32),
            pltpu.VMEM((ROWS, D), BF16),
            pltpu.SemaphoreType.DMA((N_COPIES,)),
            pltpu.SemaphoreType.DMA((N_COPIES,)),
            pltpu.SemaphoreType.DMA((N_LOADS,)),
        ],
        compiler_params=pltpu.CompilerParams(
            collective_id=0, has_side_effects=True, vmem_limit_bytes=66_000_000
        ),
        name="whole_tick",
    )(
        section_input[0], history[0], query_weight[0], key_weight[0], value_weight[0], output_weight[0],
        mix_weights,
    )
    return out[None]


def solution(mesh):
    placed = (
        P("section", "tensor", None),
        P("section", None, "tensor", None),
        P("section", None, "tensor"),
        P("section", None, "tensor"),
        P("section", None, "tensor"),
        P("section", "tensor", None),
        P(),
    )
    return jax.shard_map(
        on_device,
        mesh=mesh,
        in_specs=placed,
        out_specs=P("section", "tensor", None),
        check_vma=False,
    )
```

```python
import math

import jax
import jax.numpy as jnp
from jax import lax
from jax.experimental import pallas as pl
from jax.experimental.pallas import tpu as pltpu
from jax.sharding import PartitionSpec as P

HEAD_DIM = 64
MESH = pl.DeviceIdType.MESH
F32 = jnp.float32
BF16 = jnp.bfloat16
ROWS = 128
HALF = 64
SUB = 16
SUBS = HALF // SUB
D = 4096
SEQ = 512
QW = 768
PAIRS = QW // 128
PAIR_UNROLL = 2
KEEP = 96
QUARTER = 32
CHUNK = 1024
AGR = 0
AGL = 6
XS = 12
XT = XS + 4 * SUBS
FS = XT + 2 * SUBS
N_X = FS + 2 * SUBS
H02 = N_X
H02B = H02 + 2
H02C = H02B + 2
H01Z = H02C + 2
HZ = H01Z + 1
H01 = HZ + 1
H13 = H01 + 2
H03 = H13 + 4
H12B = H03 + 4
H12 = H12B + 2
H23 = H12 + 2
N_COPIES = H23 + 2
N_LOADS = 10


def rows_at(start, size, step):
    return pl.ds(pl.multiple_of(start, step), size)


def whole_tick(
    x_hbm, hist_hbm, wq_hbm, wk_hbm, wv_hbm, wo_hbm, mix_hbm, out_ref,
    mix, xv, xg, wqkv, wo, qkv, kc, vt, vs, heads, parts, xbuf, xtail,
    b02, b02b, b02c, b01, b13, b03, b12b, b12, b23, z01, zr, zs, hl, hm, hs, stage,
    send_sem, recv_sem, load_sem,
):
    s = lax.axis_index("section")
    x = lax.axis_index("tensor")
    y = s // 8
    zc = lax.rem(s // 4, 2)
    x_right, x_left, x_opp = lax.rem(x + 1, 4), lax.rem(x + 3, 4), lax.rem(x + 2, 4)
    right, left = (s, x_right), (s, x_left)
    up, down = (lax.rem(s + 8, 32), x), (lax.rem(s + 24, 32), x)
    pair = (s + 4 - 8 * zc, x)
    following, preceding = (lax.rem(s + 1, 32), x), (lax.rem(s + 31, 32), x)

    barrier = pltpu.get_barrier_semaphore()
    for other in (right, left, up, down, pair, following, preceding):
        pl.semaphore_signal(barrier, inc=1, device_id=other, device_id_type=MESH)

    def load(number, src, dst):
        copy = pltpu.make_async_copy(src, dst, load_sem.at[number])
        copy.start()
        return copy

    def remote(number, src, dst, device):
        return pltpu.make_async_remote_copy(
            src_ref=src,
            dst_ref=dst,
            send_sem=send_sem.at[number],
            recv_sem=recv_sem.at[number],
            device_id=device,
            device_id_type=MESH,
        )

    def send(number, src, dst, device):
        remote(number, src, dst, device).start()

    def arrived(number, ref):
        remote(number, ref, ref, pair).wait_recv()

    def left_here(number, ref):
        remote(number, ref, ref, pair).wait_send()

    def pieces(count, body):
        def step(j, carry):
            body(j)
            return carry

        lax.fori_loop(0, count, step, 0)

    columns = (1 - zc, zc)
    both = (0, 1)
    top, bottom = pl.ds(0, HALF), pl.ds(HALF, HALF)
    halves = (top, bottom)
    kept, rest = pl.ds(0, KEEP), pl.ds(KEEP, ROWS - KEEP)

    def slot(dy, i):
        return 2 * dy + columns[i] - zc - 1

    def quarter(block, q):
        return xg.at[rows_at(block * ROWS + q * QUARTER, QUARTER, QUARTER)]

    def to_right(number, block, q):
        send(AGR + number, quarter(block, q), quarter(block, q), right)

    def to_left(number, block, q):
        send(AGL + number, quarter(block, q), quarter(block, q), left)

    own = (x * ROWS, x * ROWS + HALF)
    first = (x_left * ROWS, x_right * ROWS + HALF)
    second = (
        jnp.where(x == 1, x_left * ROWS + HALF, x_opp * ROWS),
        jnp.where(x == 2, x_opp * ROWS + HALF, x_right * ROWS),
    )
    third = (
        jnp.where(x == 1, x_opp * ROWS, x_left * ROWS + HALF),
        jnp.where(x == 2, x_right * ROWS, x_opp * ROWS + HALF),
    )

    load_x = [load(0, x_hbm.at[top], xv.at[top]), load(1, x_hbm.at[bottom], xv.at[bottom])]
    for half in range(2):
        load_x[half].wait()

        def normalize_rows(j):
            r = rows_at(half * HALF + j * 16, 16, 16)
            values = xv[r, :].astype(F32)
            inv = lax.rsqrt(jnp.mean(values * values, axis=-1, keepdims=True) + 1e-05)
            xg[rows_at(x * ROWS + half * HALF + j * 16, 16, 16), :] = (values * inv).astype(BF16)

        pieces(HALF // 16, normalize_rows)
        if half == 0:
            pl.semaphore_wait(barrier, 7)
            to_right(0, x, 0)
            to_right(1, x, 1)
    to_left(2, x, 2)
    to_left(3, x, 3)

    @pl.when(x == 0)
    def _():
        to_right(2, x, 2)
        to_right(3, x, 3)

    @pl.when(x != 3)
    def _():
        to_left(0, x, 0)
        to_left(1, x, 1)

    @pl.when(y == 0)
    def _():
        for i in both:
            remote(H02 + i, hist_hbm.at[slot(2, i), kept], b02.at[i], up).start()
            remote(H02B + i, hist_hbm.at[slot(2, i), rest], b02b.at[i], down).start()
        remote(H01Z, hist_hbm.at[slot(1, 0)], z01, pair).start()

    @pl.when(y == 1)
    def _():
        for i in both:
            for h in both:
                remote(H13 + 2 * i + h, hist_hbm.at[slot(2, i), halves[h]], b13.at[i, halves[h]], down).start()
            remote(H12B + i, hist_hbm.at[slot(1, i), rest], b12b.at[i], up).start()

    @pl.when(y == 2)
    def _():
        for i in both:
            remote(H23 + i, hist_hbm.at[slot(1, i)], b23.at[i], up).start()

    @pl.when((y < 2) & (zc == 0))
    def _():
        remote(HZ, hist_hbm.at[0], zr, pair).start()

    load_w = [
        load(2, wq_hbm, wqkv.at[:, pl.ds(0, QW)]),
        load(3, wk_hbm, wqkv.at[:, pl.ds(QW, 128)]),
        load(4, wv_hbm, wqkv.at[:, pl.ds(QW + 128, 128)]),
    ]
    load_mix = load(5, mix_hbm, mix)
    far = jnp.where(y == 0, 3, 1)
    load_h = [load(6 + i, hist_hbm.at[slot(far, i)], hl.at[i]) for i in both]
    load_hm = load(8, hist_hbm.at[jnp.where(y == 0, 1, 0)], hm)
    load_wo = load(9, wo_hbm, wo)

    def weight(y_dst, c, y_src):
        return mix[2 * (y_dst - y_src) + c - zc, y_dst * 8 + c * 4 + lax.rem(s, 4)]

    def project(group):
        r0, r1 = (rows_at(start, HALF, HALF) for start in group)

        def tile(j):
            cols = rows_at(j * 256, 256, 256)
            tokens = jnp.concatenate([xg[r0, :], xg[r1, :]], axis=0)
            out = jnp.dot(tokens, wqkv[:, cols], preferred_element_type=F32).astype(BF16)
            qkv[r0, cols] = out[:HALF]
            qkv[r1, cols] = out[HALF:]

        pieces(4, tile)
        low = lax.broadcasted_iota(jnp.int32, (HALF, 128), 1) < HEAD_DIM
        for r in (r0, r1):
            keys = qkv[r, pl.ds(QW, 128)].astype(F32)
            turned = pltpu.roll(keys, HEAD_DIM, 1)
            kc[0, r, :] = jnp.where(low, keys, turned).astype(BF16)
            kc[1, r, :] = jnp.where(low, turned, keys).astype(BF16)
            vs[r, :] = qkv[r, pl.ds(QW + 128, 128)]

    exponent_scale = math.log2(math.e) / math.sqrt(HEAD_DIM)

    def attend(number, group):
        r0, r1 = (rows_at(start, HALF, HALF) for start in group)
        lane = lax.broadcasted_iota(jnp.int32, (SEQ, 2 * ROWS), 1)
        lane = jnp.where(lane < ROWS, lane, lane - ROWS)
        query = lane + jnp.where(lane < HALF, group[0], group[1] - HALF)
        seen = query >= lax.broadcasted_iota(jnp.int32, (SEQ, 2 * ROWS), 0)
        low = lax.broadcasted_iota(jnp.int32, (ROWS, 128), 1) < HEAD_DIM
        turned_values = vs[...].astype(F32).T.astype(BF16)
        vt[0] = turned_values[:HEAD_DIM]
        vt[1] = turned_values[HEAD_DIM:]

        def some_pairs(j):
            for k in range(PAIR_UNROLL):
                p = PAIR_UNROLL * j + k
                g = p // (PAIRS // 2)
                cols = rows_at(p * 128, 128, 128)
                q = jnp.concatenate([qkv[r0, cols], qkv[r1, cols]], axis=0)
                zero = jnp.zeros_like(q)
                apart = jnp.concatenate([jnp.where(low, q, zero), jnp.where(low, zero, q)], axis=0)
                scores = lax.dot_general(kc[g], apart, (((1,), (1,)), ((), ())), preferred_element_type=F32)
                scores = jnp.where(seen, scores, -1e30)
                high = jnp.max(scores, axis=0, keepdims=True)
                e = jnp.exp2((scores - high) * exponent_scale)
                total = jnp.sum(e, axis=0, keepdims=True)
                probs = (e * (1.0 / total)).astype(BF16)
                out = jnp.dot(vt[g], probs, preferred_element_type=F32)
                heads[:, cols] = jnp.concatenate([out[:, :ROWS], out[:, ROWS:]], axis=0).T.astype(BF16)

        pieces(PAIRS // PAIR_UNROLL, some_pairs)

        def tile(j):
            cols = rows_at(j * CHUNK, CHUNK, CHUNK)
            parts[number, :, cols] = jnp.dot(
                heads[...], wo[:, cols], preferred_element_type=F32
            ).astype(BF16)

        pieces(D // CHUNK, tile)

    def send_parts(number, to_left_kind, to_right_kind):
        for i in range(SUBS):
            r = pl.ds(i * SUB, SUB)
            r_low = pl.ds(HALF + i * SUB, SUB)
            send(XS + to_left_kind * SUBS + i, parts.at[number, r], xbuf.at[to_left_kind, r], left)
            send(XS + to_right_kind * SUBS + i, parts.at[number, r_low], xbuf.at[to_right_kind, r], right)

    kc[...] = jnp.zeros(kc.shape, BF16)
    vs[...] = jnp.zeros(vs.shape, BF16)
    for copy in load_w:
        copy.wait()
    project(own)

    for k in range(2):
        arrived(AGR + k, quarter(x_left, k))
        to_right(4 + k, x_left, k)
        arrived(AGL + 2 + k, quarter(x_right, 2 + k))
        to_left(4 + k, x_right, 2 + k)

    @pl.when(x != 0)
    def _():
        to_right(2, x, 2)
        to_right(3, x, 3)

    @pl.when(x == 3)
    def _():
        to_left(0, x, 0)
        to_left(1, x, 1)

    load_mix.wait()
    for copy in load_h:
        copy.wait()
    load_hm.wait()

    def merge(count, dst, theirs, mine_weight, mine):
        def rows(j):
            r = rows_at(j * 16, 16, 16)
            dst[r, :] = (theirs * dst[r, :].astype(F32) + mine_weight * mine[r, :].astype(F32)).astype(BF16)

        pieces(count // 16, rows)

    def far_sum(i, h):
        arrived(H13 + 2 * i + h, b13.at[i, halves[h]])
        merge(HALF, b13.at[i, halves[h]], weight(3, columns[i], 1), weight(3, columns[i], 0), hl.at[i, halves[h]])
        remote(H03 + 2 * i + h, b13.at[i, halves[h]], b03.at[i, halves[h]], down).start()

    def near_sum(i):
        arrived(H02 + i, b02.at[i])
        merge(KEEP, b02.at[i], weight(2, columns[i], 0), weight(2, columns[i], 1), hl.at[i, kept])
        remote(H12 + i, b02.at[i], b12.at[i], up).start()

    def column_sum(i, add):
        c = columns[i]

        @pl.when(y == 2)
        def _():
            arrived(H12 + i, b12.at[i])
            arrived(H12B + i, b12b.at[i])
            arrived(H02C + i, b02c.at[i])
            one, two = weight(2, c, 1), weight(2, c, 0)

            def upper(j):
                r = rows_at(j * 16, 16, 16)
                add(r, b12[i, r, :].astype(F32))

            def lower(j):
                r = rows_at(j * 16, 16, 16)
                add(
                    rows_at(KEEP + j * 16, 16, 16),
                    one * b12b[i, r, :].astype(F32) + two * b02c[i, r, :].astype(F32),
                )

            pieces(KEEP // 16, upper)
            pieces((ROWS - KEEP) // 16, lower)

        @pl.when(y == 3)
        def _():
            for h in both:
                arrived(H03 + 2 * i + h, b03.at[i, halves[h]])
            arrived(H23 + i, b23.at[i])
            one = weight(3, c, 2)

            def every(j):
                r = rows_at(j * 16, 16, 16)
                add(r, b03[i, r, :].astype(F32) + one * b23[i, r, :].astype(F32))

            pieces(ROWS // 16, every)

    @pl.when(y == 0)
    def _():
        far_sum(0, 0)

    @pl.when(y == 3)
    def _():
        for i in both:
            arrived(H02B + i, b02b.at[i])
            remote(H02C + i, b02b.at[i], b02c.at[i], down).start()

    project(first)

    def group_arrived(from_left, from_right):
        for k in range(2):
            arrived(AGR + from_left + k, quarter(x, k))
            arrived(AGL + from_right + k, quarter(x, k))

    left_2 = jnp.where(x == 1, 2, 4)
    right_2 = jnp.where(x == 2, 4, 0)
    group_arrived(left_2, right_2)
    project(second)

    @pl.when(y == 0)
    def _():
        far_sum(0, 1)

    @pl.when(y == 1)
    def _():
        near_sum(0)

    load_wo.wait()
    attend(2, second)
    left_kind = jnp.where(x == 1, 2, 0)
    right_kind = jnp.where(x == 2, 1, 3)
    send_parts(2, left_kind, right_kind)

    group_arrived(6 - left_2, 4 - right_2)
    project(third)

    @pl.when(y == 0)
    def _():
        far_sum(1, 0)

    nearest_pair = jnp.where(zc == 0, mix[1, jnp.minimum(s + 4, 31)], F32(0.0))

    def for_pair(r, value):
        zs[r, :] = (value + nearest_pair * hm[r, :].astype(F32)).astype(BF16)

    column_sum(0, for_pair)

    @pl.when(y >= 2)
    def _():
        remote(HZ, zs, zr, pair).start()

    attend(3, third)
    send_parts(3, 2 - left_kind, 4 - right_kind)

    @pl.when(y == 0)
    def _():
        arrived(H01Z, z01)
        for h in both:
            merge(HALF, z01.at[halves[h]], mix[2 + zc - (1 - zc), s + 8], weight(1, zc, 0), hm.at[halves[h]])
            remote(H01 + h, z01.at[halves[h]], b01.at[halves[h]], up).start()

    @pl.when(y == 1)
    def _():
        near_sum(1)

    attend(1, first)

    @pl.when(y == 0)
    def _():
        far_sum(1, 1)

    attend(0, own)

    for i in range(SUBS):
        r = pl.ds(i * SUB, SUB)
        r_low = pl.ds(HALF + i * SUB, SUB)
        arrived(XS + i, xbuf.at[0, r])
        parts[1, r, :] = (parts[1, r, :].astype(F32) + xbuf[0, r, :].astype(F32)).astype(BF16)
        send(XT + i, parts.at[1, r], xtail.at[0, r], left)
        arrived(XS + SUBS + i, xbuf.at[1, r])
        parts[1, r_low, :] = (parts[1, r_low, :].astype(F32) + xbuf[1, r, :].astype(F32)).astype(BF16)
        send(XT + SUBS + i, parts.at[1, r_low], xtail.at[1, r], right)

    def with_pair(r, value):
        hs[r, :] = value + zr[r, :].astype(F32)

    @pl.when((y >= 2) | (zc == 1))
    def _():
        arrived(HZ, zr)

    column_sum(1, with_pair)
    nearest = mix[1, s]

    def every_row(body):
        pieces(ROWS // 16, lambda j: body(rows_at(j * 16, 16, 16)))

    @pl.when(y == 0)
    def _():
        def nothing(r):
            hs[r, :] = jnp.zeros((16, D), F32)

        every_row(nothing)

    @pl.when(y == 1)
    def _():
        for h in both:
            arrived(H01 + h, b01.at[halves[h]])

        def from_row_0(r):
            hs[r, :] = b01[r, :].astype(F32)

        every_row(from_row_0)

    @pl.when((y < 2) & (zc == 1))
    def _():
        def from_pair(r):
            hs[r, :] = hs[r, :] + nearest * zr[r, :].astype(F32)

        every_row(from_pair)

    for i in range(2 * SUBS):
        arrived(XS + 2 * SUBS + i, xbuf.at[2, pl.ds(0, SUB)])
    own_weight = mix[0, s]
    for i in range(SUBS):
        r = pl.ds(i * SUB, SUB)
        for side in range(2):
            rr = pl.ds(side * HALF + i * SUB, SUB)
            arrived(XT + side * SUBS + i, xtail.at[side, r])

            def mix_columns(j):
                cols = rows_at(j * 1024, 1024, 1024)
                total = (
                    parts[0, rr, cols].astype(F32)
                    + xtail[side, r, cols].astype(F32)
                    + xbuf[3 - side, r, cols].astype(F32)
                )
                block_out = (xv[rr, cols].astype(F32) + total).astype(BF16)
                stage[rr, cols] = (own_weight * block_out.astype(F32) + hs[rr, cols]).astype(BF16)

            pieces(D // 1024, mix_columns)
            send(FS + side * SUBS + i, stage.at[rr], out_ref.at[rr], following)

    @pl.when(y == 0)
    def _():
        for i in both:
            left_here(H02 + i, b02.at[i])
            left_here(H02B + i, b02b.at[i])
            left_here(H01 + i, z01.at[halves[i]])
            for h in both:
                left_here(H03 + 2 * i + h, b13.at[i, halves[h]])
        left_here(H01Z, z01)

    @pl.when(y == 1)
    def _():
        for i in both:
            for h in both:
                left_here(H13 + 2 * i + h, b13.at[i, halves[h]])
            left_here(H12B + i, b12b.at[i])
            left_here(H12 + i, b02.at[i])

    @pl.when(y == 2)
    def _():
        for i in both:
            left_here(H23 + i, b23.at[i])

    @pl.when(y == 3)
    def _():
        for i in both:
            left_here(H02C + i, b02b.at[i])

    @pl.when((y >= 2) | (zc == 0))
    def _():
        left_here(HZ, zr)

    for number in range(12):
        left_here(number, quarter(x, 0))
    for number in range(XS, N_X):
        left_here(number, stage.at[pl.ds(0, SUB)])
    for i in range(2 * SUBS):
        arrived(FS + i, out_ref.at[pl.ds(i * SUB, SUB)])


def on_device(section_input, history, query_weight, key_weight, value_weight, output_weight, mix_weights):
    anywhere = pl.BlockSpec(memory_space=pl.ANY)
    block = (ROWS, D)
    out = pl.pallas_call(
        whole_tick,
        out_shape=jax.ShapeDtypeStruct(block, BF16),
        in_specs=[anywhere] * 7,
        out_specs=anywhere,
        scratch_shapes=[
            pltpu.SMEM((8, 32), F32),
            pltpu.VMEM(block, BF16),
            pltpu.VMEM((SEQ, D), BF16),
            pltpu.VMEM((D, QW + 256), BF16),
            pltpu.VMEM((QW, D), BF16),
            pltpu.VMEM((SEQ, QW + 256), BF16),
            pltpu.VMEM((2, SEQ, 128), BF16),
            pltpu.VMEM((2, HEAD_DIM, SEQ), BF16),
            pltpu.VMEM((SEQ, 128), BF16),
            pltpu.VMEM((ROWS, QW), BF16),
            pltpu.VMEM((4, ROWS, D), BF16),
            pltpu.VMEM((4, HALF, D), BF16),
            pltpu.VMEM((2, HALF, D), BF16),
            pltpu.VMEM((2, KEEP, D), BF16),
            pltpu.VMEM((2, ROWS - KEEP, D), BF16),
            pltpu.VMEM((2, ROWS - KEEP, D), BF16),
            pltpu.VMEM(block, BF16),
            pltpu.VMEM((2, ROWS, D), BF16),
            pltpu.VMEM((2, ROWS, D), BF16),
            pltpu.VMEM((2, ROWS - KEEP, D), BF16),
            pltpu.VMEM((2, KEEP, D), BF16),
            pltpu.VMEM((2, ROWS, D), BF16),
            pltpu.VMEM(block, BF16),
            pltpu.VMEM(block, BF16),
            pltpu.VMEM(block, BF16),
            pltpu.VMEM((2, ROWS, D), BF16),
            pltpu.VMEM(block, BF16),
            pltpu.VMEM(block, F32),
            pltpu.VMEM(block, BF16),
            pltpu.SemaphoreType.DMA((N_COPIES,)),
            pltpu.SemaphoreType.DMA((N_COPIES,)),
            pltpu.SemaphoreType.DMA((N_LOADS,)),
        ],
        compiler_params=pltpu.CompilerParams(
            collective_id=0, has_side_effects=True, vmem_limit_bytes=64_000_000
        ),
        name="whole_tick",
    )(
        section_input[0], history[0], query_weight[0], key_weight[0], value_weight[0], output_weight[0],
        mix_weights.T,
    )
    return out[None]


def solution(mesh):
    placed = (
        P("section", "tensor", None),
        P("section", None, "tensor", None),
        P("section", None, "tensor"),
        P("section", None, "tensor"),
        P("section", None, "tensor"),
        P("section", "tensor", None),
        P(),
    )
    return jax.shard_map(
        on_device,
        mesh=mesh,
        in_specs=placed,
        out_specs=P("section", "tensor", None),
        check_vma=False,
    )
```

```python
import math

import jax
import jax.numpy as jnp
from jax import lax
from jax.experimental import pallas as pl
from jax.experimental.pallas import tpu as pltpu
from jax.sharding import PartitionSpec as P

HEAD_DIM = 64
MESH = pl.DeviceIdType.MESH
F32 = jnp.float32
BF16 = jnp.bfloat16
ROWS = 128
HALF = 64
D = 4096
SEQ = 512
QW = 768
PAIRS = QW // 128
PAIR_UNROLL = 2
KEEP = 96
QUARTER = 32
CHUNK = 1024
PIECES = ((0, 0, D), (16, 0, D), (32, 0, D), (48, 0, D // 2), (48, D // 2, D // 2))
SUB = 16
N_P = len(PIECES)
AGR, AGL = 0, 4
XS = 8
XT = XS + 2 * N_P + 2
FS = XT + 2 * N_P
HZ = FS + 1
H = HZ + 2
H13, H01Z = H, H + 4
H02, H01 = H, H + 4
H12, H12B, H02C = H, H + 4, H + 6
H03, H23, H02B = H, H + 4, H + 8
N_ARRIVALS = H + 10
O_AG, O_XS, O_XT, O_FS, O_HZ, O_H = 0, 1, 2, 3, 4, 5
N_LEAVING = O_H + 3
N_LOADS = 8


def rows_at(start, size, step):
    return pl.ds(pl.multiple_of(start, step), size)


def whole_tick(
    x_hbm, hist_hbm, wq_hbm, wk_hbm, wv_hbm, wo_hbm, mix_hbm, out_ref,
    mix, xv, xg, wqkv, wo, qkv, kc, vt, vs, heads, parts, xbuf, xtail,
    b02, b02b, b02c, b01, b13, b03, b12b, b12, b23, z01, zr, zs, hl, hm, hs, stage,
    send_sem, recv_sem, load_sem,
):
    s = lax.axis_index("section")
    x = lax.axis_index("tensor")
    y = s // 8
    zc = lax.rem(s // 4, 2)
    x_right, x_left, x_opp = lax.rem(x + 1, 4), lax.rem(x + 3, 4), lax.rem(x + 2, 4)
    right, left = (s, x_right), (s, x_left)
    up, down = (lax.rem(s + 8, 32), x), (lax.rem(s + 24, 32), x)
    pair = (s + 4 - 8 * zc, x)
    following, preceding = (lax.rem(s + 1, 32), x), (lax.rem(s + 31, 32), x)

    barrier = pltpu.get_barrier_semaphore()
    for other in (right, left, up, down, pair, following, preceding):
        pl.semaphore_signal(barrier, inc=1, device_id=other, device_id_type=MESH)

    def load(number, src, dst):
        copy = pltpu.make_async_copy(src, dst, load_sem.at[number])
        copy.start()
        return copy

    def remote(leaving, number, src, dst, device):
        return pltpu.make_async_remote_copy(
            src_ref=src,
            dst_ref=dst,
            send_sem=send_sem.at[leaving],
            recv_sem=recv_sem.at[number],
            device_id=device,
            device_id_type=MESH,
        )

    def send(leaving, number, src, dst, device):
        remote(leaving, number, src, dst, device).start()

    def arrived(number, ref):
        remote(0, number, ref, ref, pair).wait_recv()

    def left_here(leaving, ref):
        remote(leaving, 0, ref, ref, pair).wait_send()

    def pieces(count, body):
        def step(j, carry):
            body(j)
            return carry

        lax.fori_loop(0, count, step, 0)

    columns = (1 - zc, zc)
    both = (0, 1)
    top, bottom = pl.ds(0, HALF), pl.ds(HALF, HALF)
    halves = (top, bottom)
    rest = pl.ds(KEEP, ROWS - KEEP)
    kept = (top, pl.ds(HALF, KEEP - HALF))

    def slot(dy, i):
        return 2 * dy + columns[i] - zc - 1

    def quarter(block, q):
        return xg.at[rows_at(block * ROWS + q * QUARTER, QUARTER, QUARTER)]

    def to_right(number, block, q):
        send(O_AG, AGR + number, quarter(block, q), quarter(block, q), right)

    def to_left(number, block, q):
        send(O_AG, AGL + number, quarter(block, q), quarter(block, q), left)

    own = (x * ROWS, x * ROWS + HALF)
    first = (x_left * ROWS, x_right * ROWS + HALF)
    second = (
        jnp.where(x == 1, x_left * ROWS + HALF, x_opp * ROWS),
        jnp.where(x == 2, x_opp * ROWS + HALF, x_right * ROWS),
    )
    third = (
        jnp.where(x == 1, x_opp * ROWS, x_left * ROWS + HALF),
        jnp.where(x == 2, x_right * ROWS, x_opp * ROWS + HALF),
    )

    order = (0, 2, 1, 3)
    load_x = []
    for n, q in enumerate(order):
        r = pl.ds(q * QUARTER, QUARTER)
        load_x.append(load(n, x_hbm.at[r], xv.at[r]))
    for n, q in enumerate(order):
        load_x[n].wait()

        def normalize_rows(j):
            r = rows_at(q * QUARTER + j * 16, 16, 16)
            values = xv[r, :].astype(F32)
            inv = lax.rsqrt(jnp.mean(values * values, axis=-1, keepdims=True) + 1e-05)
            xg[rows_at(x * ROWS + q * QUARTER + j * 16, 16, 16), :] = (values * inv).astype(BF16)

        pieces(QUARTER // 16, normalize_rows)
        if n == 0:
            pl.semaphore_wait(barrier, 7)
        if q < 2:
            to_right(q, x, q)
        else:
            to_left(q - 2, x, q)

    @pl.when(x == 0)
    def _():
        to_right(2, x, 2)
        to_right(2, x, 3)

    @pl.when(x != 3)
    def _():
        to_left(2, x, 0)
        to_left(2, x, 1)

    @pl.when(y == 0)
    def _():
        for i in both:
            for h in both:
                remote(O_H, H02 + 2 * i + h, hist_hbm.at[slot(2, i), kept[h]], b02.at[i, kept[h]], up).start()
            remote(O_H, H02B + i, hist_hbm.at[slot(2, i), rest], b02b.at[i], down).start()
        remote(O_H + 2, H01Z, hist_hbm.at[slot(1, 0)], z01, pair).start()

    @pl.when(y == 1)
    def _():
        for i in both:
            for h in both:
                remote(O_H, H13 + 2 * i + h, hist_hbm.at[slot(2, i), halves[h]], b13.at[i, halves[h]], down).start()
            remote(O_H + 1, H12B + i, hist_hbm.at[slot(1, i), rest], b12b.at[i], up).start()

    @pl.when(y == 2)
    def _():
        for i in both:
            for h in both:
                remote(O_H, H23 + 2 * i + h, hist_hbm.at[slot(1, i), halves[h]], b23.at[i, halves[h]], up).start()

    @pl.when((y < 2) & (zc == 0))
    def _():
        for h in both:
            remote(O_HZ, HZ + h, hist_hbm.at[0, halves[h]], zr.at[halves[h]], pair).start()

    load_w = [
        load(4, wq_hbm, wqkv.at[:, pl.ds(0, QW)]),
        load(5, wk_hbm, wqkv.at[:, pl.ds(QW, 128)]),
        load(6, wv_hbm, wqkv.at[:, pl.ds(QW + 128, 128)]),
    ]
    load_mix = load(7, mix_hbm, mix)
    far = jnp.where(y == 0, 3, 1)
    load_h = [load(i, hist_hbm.at[slot(far, i)], hl.at[i]) for i in both]
    load_hm = load(2, hist_hbm.at[jnp.where(y == 0, 1, 0)], hm)
    load_wo = load(3, wo_hbm, wo)

    def weight(y_dst, c, y_src):
        return mix[2 * (y_dst - y_src) + c - zc, y_dst * 8 + c * 4 + lax.rem(s, 4)]

    def project(group):
        r0, r1 = (rows_at(start, HALF, HALF) for start in group)

        def tile(j):
            cols = rows_at(j * 256, 256, 256)
            tokens = jnp.concatenate([xg[r0, :], xg[r1, :]], axis=0)
            out = jnp.dot(tokens, wqkv[:, cols], preferred_element_type=F32).astype(BF16)
            qkv[r0, cols] = out[:HALF]
            qkv[r1, cols] = out[HALF:]

        pieces(4, tile)
        low = lax.broadcasted_iota(jnp.int32, (HALF, 128), 1) < HEAD_DIM
        for r in (r0, r1):
            keys = qkv[r, pl.ds(QW, 128)].astype(F32)
            turned = pltpu.roll(keys, HEAD_DIM, 1)
            kc[0, r, :] = jnp.where(low, keys, turned).astype(BF16)
            kc[1, r, :] = jnp.where(low, turned, keys).astype(BF16)
            vs[r, :] = qkv[r, pl.ds(QW + 128, 128)]

    exponent_scale = math.log2(math.e) / math.sqrt(HEAD_DIM)

    def attend(number, group):
        r0, r1 = (rows_at(start, HALF, HALF) for start in group)
        lane = lax.broadcasted_iota(jnp.int32, (SEQ, 2 * ROWS), 1)
        lane = jnp.where(lane < ROWS, lane, lane - ROWS)
        query = lane + jnp.where(lane < HALF, group[0], group[1] - HALF)
        seen = query >= lax.broadcasted_iota(jnp.int32, (SEQ, 2 * ROWS), 0)
        low = lax.broadcasted_iota(jnp.int32, (ROWS, 128), 1) < HEAD_DIM
        turned_values = vs[...].astype(F32).T.astype(BF16)
        vt[0] = turned_values[:HEAD_DIM]
        vt[1] = turned_values[HEAD_DIM:]

        def some_pairs(j):
            for k in range(PAIR_UNROLL):
                p = PAIR_UNROLL * j + k
                g = p // (PAIRS // 2)
                cols = rows_at(p * 128, 128, 128)
                q = jnp.concatenate([qkv[r0, cols], qkv[r1, cols]], axis=0)
                zero = jnp.zeros_like(q)
                apart = jnp.concatenate([jnp.where(low, q, zero), jnp.where(low, zero, q)], axis=0)
                scores = lax.dot_general(kc[g], apart, (((1,), (1,)), ((), ())), preferred_element_type=F32)
                scores = jnp.where(seen, scores, -1e30)
                high = jnp.max(scores, axis=0, keepdims=True)
                e = jnp.exp2((scores - high) * exponent_scale)
                total = jnp.sum(e, axis=0, keepdims=True)
                probs = (e * (1.0 / total)).astype(BF16)
                out = jnp.dot(vt[g], probs, preferred_element_type=F32)
                heads[:, cols] = jnp.concatenate([out[:, :ROWS], out[:, ROWS:]], axis=0).T.astype(BF16)

        pieces(PAIRS // PAIR_UNROLL, some_pairs)

        def tile(j):
            cols = rows_at(j * CHUNK, CHUNK, CHUNK)
            parts[number, :, cols] = jnp.dot(
                heads[...], wo[:, cols], preferred_element_type=F32
            ).astype(BF16)

        pieces(D // CHUNK, tile)

    def piece(i, ref, first_row=0):
        row, column, width = PIECES[i]
        return ref.at[pl.ds(first_row + row, SUB), pl.ds(column, width)]

    def send_parts(number, to_left_kind, to_right_kind):
        for i in range(N_P):
            send(
                O_XS,
                XS + jnp.where(to_left_kind == 0, i, 2 * N_P),
                piece(i, parts.at[number]),
                piece(i, xbuf.at[to_left_kind]),
                left,
            )
            send(
                O_XS,
                XS + jnp.where(to_right_kind == 1, N_P + i, 2 * N_P + 1),
                piece(i, parts.at[number], HALF),
                piece(i, xbuf.at[to_right_kind]),
                right,
            )

    kc[...] = jnp.zeros(kc.shape, BF16)
    vs[...] = jnp.zeros(vs.shape, BF16)
    for copy in load_w:
        copy.wait()
    project(own)

    for k in range(2):
        arrived(AGR + k, quarter(x_left, k))
        to_right(3, x_left, k)
        arrived(AGL + k, quarter(x_right, 2 + k))
        to_left(3, x_right, 2 + k)

    @pl.when(x != 0)
    def _():
        to_right(2, x, 2)
        to_right(2, x, 3)

    @pl.when(x == 3)
    def _():
        to_left(2, x, 0)
        to_left(2, x, 1)

    load_mix.wait()
    for copy in load_h:
        copy.wait()
    load_hm.wait()

    def merge(count, dst, theirs, mine_weight, mine):
        def rows(j):
            r = rows_at(j * 16, 16, 16)
            dst[r, :] = (theirs * dst[r, :].astype(F32) + mine_weight * mine[r, :].astype(F32)).astype(BF16)

        pieces(count // 16, rows)

    def far_sum(i, h):
        arrived(H13 + 2 * i + h, b13.at[i, halves[h]])
        merge(HALF, b13.at[i, halves[h]], weight(3, columns[i], 1), weight(3, columns[i], 0), hl.at[i, halves[h]])
        remote(O_H + 1, H03 + 2 * i + h, b13.at[i, halves[h]], b03.at[i, halves[h]], down).start()

    def near_sum(i, h):
        n, rows = 2 * i + h, b02.at[i, kept[h]]
        arrived(H02 + n, rows)
        merge(
            (HALF, KEEP - HALF)[h], rows, weight(2, columns[i], 0), weight(2, columns[i], 1), hl.at[i, kept[h]]
        )
        remote(O_H + 1, H12 + n, rows, b12.at[i, kept[h]], up).start()

    def column_sum(i, h, add):
        c = columns[i]

        @pl.when(y == 2)
        def _():
            arrived(H12 + 2 * i + h, b12.at[i, kept[h]])

            def upper(j):
                r = rows_at(h * HALF + j * 16, 16, 16)
                add(r, b12[i, r, :].astype(F32))

            pieces((HALF, KEEP - HALF)[h] // 16, upper)
            if h == 1:
                arrived(H12B + i, b12b.at[i])
                arrived(H02C + i, b02c.at[i])
                one, two = weight(2, c, 1), weight(2, c, 0)

                def lower(j):
                    r = rows_at(j * 16, 16, 16)
                    add(
                        rows_at(KEEP + j * 16, 16, 16),
                        one * b12b[i, r, :].astype(F32) + two * b02c[i, r, :].astype(F32),
                    )

                pieces((ROWS - KEEP) // 16, lower)

        @pl.when(y == 3)
        def _():
            arrived(H03 + 2 * i + h, b03.at[i, halves[h]])
            arrived(H23 + 2 * i + h, b23.at[i, halves[h]])
            one = weight(3, c, 2)

            def every(j):
                r = rows_at(h * HALF + j * 16, 16, 16)
                add(r, b03[i, r, :].astype(F32) + one * b23[i, r, :].astype(F32))

            pieces(HALF // 16, every)

    nearest_pair = jnp.where(zc == 0, mix[1, jnp.minimum(s + 4, 31)], F32(0.0))

    def for_pair(r, value):
        zs[r, :] = (value + nearest_pair * hm[r, :].astype(F32)).astype(BF16)

    def to_pair(h):
        column_sum(0, h, for_pair)

        @pl.when(y >= 2)
        def _():
            remote(O_HZ, HZ + h, zs.at[halves[h]], zr.at[halves[h]], pair).start()

    @pl.when(y == 0)
    def _():
        far_sum(0, 0)

    @pl.when(y == 3)
    def _():
        for i in both:
            arrived(H02B + i, b02b.at[i])
            remote(O_H, H02C + i, b02b.at[i], b02c.at[i], down).start()

    @pl.when(y == 1)
    def _():
        near_sum(0, 0)

    project(first)

    def group_arrived(from_left, from_right):
        arrived(AGR + from_left, xg.at[top])
        arrived(AGL + from_right, xg.at[top])

    @pl.when(y == 1)
    def _():
        near_sum(0, 1)

    @pl.when(y == 0)
    def _():
        far_sum(0, 1)

    left_2 = jnp.where(x == 1, 2, 3)
    right_2 = jnp.where(x == 2, 3, 2)
    group_arrived(left_2, right_2)
    project(second)
    to_pair(0)

    @pl.when(y == 0)
    def _():
        arrived(H01Z, z01)
        for h in both:
            merge(HALF, z01.at[halves[h]], mix[2 + zc - (1 - zc), s + 8], weight(1, zc, 0), hm.at[halves[h]])
            remote(O_H + 2, H01 + h, z01.at[halves[h]], b01.at[halves[h]], up).start()

    load_wo.wait()
    attend(2, second)
    left_kind = jnp.where(x == 1, 2, 0)
    right_kind = jnp.where(x == 2, 1, 3)
    send_parts(2, left_kind, right_kind)

    @pl.when(y == 0)
    def _():
        far_sum(1, 0)

    @pl.when(y == 1)
    def _():
        near_sum(1, 0)

    group_arrived(5 - left_2, 5 - right_2)
    project(third)
    to_pair(1)

    @pl.when(y == 1)
    def _():
        near_sum(1, 1)

    attend(3, third)
    send_parts(3, 2 - left_kind, 4 - right_kind)

    @pl.when(y == 0)
    def _():
        far_sum(1, 1)

    attend(1, first)
    attend(0, own)

    for i in range(N_P):
        row, column, width = PIECES[i]
        cols = pl.ds(column, width)
        for side in both:
            r, rr = pl.ds(row, SUB), pl.ds(side * HALF + row, SUB)
            arrived(XS + side * N_P + i, piece(i, xbuf.at[side]))
            parts[1, rr, cols] = (
                parts[1, rr, cols].astype(F32) + xbuf[side, r, cols].astype(F32)
            ).astype(BF16)
            send(
                O_XT,
                XT + side * N_P + i,
                piece(i, parts.at[1], side * HALF),
                piece(i, xtail.at[side]),
                (left, right)[side],
            )

    def with_pair(r, value):
        hs[r, :] = value + zr[r, :].astype(F32)

    @pl.when((y >= 2) | (zc == 1))
    def _():
        for h in both:
            arrived(HZ + h, zr.at[halves[h]])

    for h in both:
        column_sum(1, h, with_pair)
    nearest = mix[1, s]

    def every_row(body):
        pieces(ROWS // 16, lambda j: body(rows_at(j * 16, 16, 16)))

    @pl.when(y == 0)
    def _():
        def nothing(r):
            hs[r, :] = jnp.zeros((16, D), F32)

        every_row(nothing)

    @pl.when(y == 1)
    def _():
        for h in both:
            arrived(H01 + h, b01.at[halves[h]])

        def from_row_0(r):
            hs[r, :] = b01[r, :].astype(F32)

        every_row(from_row_0)

    @pl.when((y < 2) & (zc == 1))
    def _():
        def from_pair(r):
            hs[r, :] = hs[r, :] + nearest * zr[r, :].astype(F32)

        every_row(from_pair)

    arrived(XS + 2 * N_P, xbuf.at[2])
    arrived(XS + 2 * N_P + 1, xbuf.at[3])
    own_weight = mix[0, s]
    for i in range(N_P):
        row, column, width = PIECES[i]
        for side in both:
            r, rr = pl.ds(row, SUB), pl.ds(side * HALF + row, SUB)
            arrived(XT + side * N_P + i, piece(i, xtail.at[side]))

            def mix_columns(j):
                cols = rows_at(column + j * 1024, 1024, 1024)
                total = (
                    parts[0, rr, cols].astype(F32)
                    + xtail[side, r, cols].astype(F32)
                    + xbuf[3 - side, r, cols].astype(F32)
                )
                block_out = (xv[rr, cols].astype(F32) + total).astype(BF16)
                stage[rr, cols] = (own_weight * block_out.astype(F32) + hs[rr, cols]).astype(BF16)

            pieces(width // 1024, mix_columns)
            send(O_FS, FS, piece(i, stage, side * HALF), piece(i, out_ref, side * HALF), following)

    def many(rows):
        return xg.at[pl.ds(0, rows)]

    left_here(O_AG, many(3 * ROWS))
    left_here(O_XS, many(2 * ROWS))

    @pl.when(y < 3)
    def _():
        left_here(O_H, many(2 * ROWS))

    @pl.when(y == 3)
    def _():
        left_here(O_H, many(2 * (ROWS - KEEP)))

    @pl.when(y < 2)
    def _():
        left_here(O_H + 1, many(2 * ROWS))

    @pl.when(y == 0)
    def _():
        left_here(O_H + 2, many(2 * ROWS))

    @pl.when((y >= 2) | (zc == 0))
    def _():
        left_here(O_HZ, many(ROWS))

    left_here(O_XT, many(ROWS))
    left_here(O_FS, stage)
    arrived(FS, out_ref)


def on_device(section_input, history, query_weight, key_weight, value_weight, output_weight, mix_weights):
    anywhere = pl.BlockSpec(memory_space=pl.ANY)
    block = (ROWS, D)
    out = pl.pallas_call(
        whole_tick,
        out_shape=pltpu.VMEM(block, BF16),
        in_specs=[anywhere] * 7,
        out_specs=pl.BlockSpec(memory_space=pltpu.VMEM),
        scratch_shapes=[
            pltpu.SMEM((8, 32), F32),
            pltpu.VMEM(block, BF16),
            pltpu.VMEM((SEQ, D), BF16),
            pltpu.VMEM((D, QW + 256), BF16),
            pltpu.VMEM((QW, D), BF16),
            pltpu.VMEM((SEQ, QW + 256), BF16),
            pltpu.VMEM((2, SEQ, 128), BF16),
            pltpu.VMEM((2, HEAD_DIM, SEQ), BF16),
            pltpu.VMEM((SEQ, 128), BF16),
            pltpu.VMEM((ROWS, QW), BF16),
            pltpu.VMEM((4, ROWS, D), BF16),
            pltpu.VMEM((4, HALF, D), BF16),
            pltpu.VMEM((2, HALF, D), BF16),
            pltpu.VMEM((2, KEEP, D), BF16),
            pltpu.VMEM((2, ROWS - KEEP, D), BF16),
            pltpu.VMEM((2, ROWS - KEEP, D), BF16),
            pltpu.VMEM(block, BF16),
            pltpu.VMEM((2, ROWS, D), BF16),
            pltpu.VMEM((2, ROWS, D), BF16),
            pltpu.VMEM((2, ROWS - KEEP, D), BF16),
            pltpu.VMEM((2, KEEP, D), BF16),
            pltpu.VMEM((2, ROWS, D), BF16),
            pltpu.VMEM(block, BF16),
            pltpu.VMEM(block, BF16),
            pltpu.VMEM(block, BF16),
            pltpu.VMEM((2, ROWS, D), BF16),
            pltpu.VMEM(block, BF16),
            pltpu.VMEM(block, F32),
            pltpu.VMEM(block, BF16),
            pltpu.SemaphoreType.DMA((N_LEAVING,)),
            pltpu.SemaphoreType.DMA((N_ARRIVALS,)),
            pltpu.SemaphoreType.DMA((N_LOADS,)),
        ],
        compiler_params=pltpu.CompilerParams(
            collective_id=0, has_side_effects=True, vmem_limit_bytes=60_000_000
        ),
        name="whole_tick",
    )(
        section_input[0], history[0], query_weight[0], key_weight[0], value_weight[0], output_weight[0],
        mix_weights.T,
    )
    return out[None]


def solution(mesh):
    placed = (
        P("section", "tensor", None),
        P("section", None, "tensor", None),
        P("section", None, "tensor"),
        P("section", None, "tensor"),
        P("section", None, "tensor"),
        P("section", "tensor", None),
        P(),
    )
    return jax.shard_map(
        on_device,
        mesh=mesh,
        in_specs=placed,
        out_specs=P("section", "tensor", None),
        check_vma=False,
    )
```

```python
import math

import jax
import jax.numpy as jnp
from jax import lax
from jax.experimental import pallas as pl
from jax.experimental.pallas import tpu as pltpu
from jax.sharding import PartitionSpec as P

HEAD_DIM = 64
MESH = pl.DeviceIdType.MESH
F32 = jnp.float32
BF16 = jnp.bfloat16
ROWS = 128
HALF = 64
D = 4096
SEQ = 512
QW = 768
PAIRS = QW // 128
PAIR_UNROLL = 2
KEEP = 96
QUARTER = 32
FAR = ((0, 0, 32), (0, 32, 32), (0, HALF, HALF), (1, 0, HALF), (1, HALF, HALF))
CHUNK = 1024
SUB = 16
WIDTH = D // 2
N_P = HALF // SUB
N_T = N_P * D // WIDTH
AGR, AGL = 0, 4
XS = 8
XT = XS + 2 * N_P + 2
FS = XT + 2 * N_T
HZ = FS + 1
H = HZ + 2
H13, H01Z = H, H + 5
H02, H01 = H, H + 4
H12, H12B, H02C = H, H + 4, H + 6
H03, H23, H02B = H, H + 5, H + 9
N_ARRIVALS = H + 11
O_AG, O_XS, O_XT, O_FS, O_HZ, O_H = 0, 1, 2, 3, 4, 5
N_LEAVING = O_H + 3
N_LOADS = 8


def rows_at(start, size, step):
    return pl.ds(pl.multiple_of(start, step), size)


def whole_tick(
    x_hbm, hist_hbm, wq_hbm, wk_hbm, wv_hbm, wo_hbm, mix_hbm, out_ref,
    mix, xv, xg, wqkv, wo, qkv, kc, vt, vs, heads, parts, xbuf, xtail,
    b02, b02b, b02c, b01, b13, b03, b12b, b12, b23, z01, zr, zs, hl, hm, hs, stage,
    send_sem, recv_sem, load_sem,
):
    def load(number, src, dst):
        copy = pltpu.make_async_copy(src, dst, load_sem.at[number])
        copy.start()
        return copy

    order = (0, 2, 1, 3)
    load_x = []
    for n, q in enumerate(order):
        r = pl.ds(q * QUARTER, QUARTER)
        load_x.append(load(n, x_hbm.at[r], xv.at[r]))

    s = lax.axis_index("section")
    x = lax.axis_index("tensor")
    core = lax.rem(s, 2)
    y = s // 8
    zc = lax.rem(s // 4, 2)
    x_right, x_left, x_opp = lax.rem(x + 1, 4), lax.rem(x + 3, 4), lax.rem(x + 2, 4)
    right, left = (s, x_right), (s, x_left)
    up, down = (lax.rem(s + 8, 32), x), (lax.rem(s + 24, 32), x)
    pair = (s + 4 - 8 * zc, x)
    following, preceding = (lax.rem(s + 1, 32), x), (lax.rem(s + 31, 32), x)

    barrier = pltpu.get_barrier_semaphore()
    for other in (right, left, up, down, pair, following, preceding):
        pl.semaphore_signal(barrier, inc=1, device_id=other, device_id_type=MESH)

    def remote(leaving, number, src, dst, device):
        return pltpu.make_async_remote_copy(
            src_ref=src,
            dst_ref=dst,
            send_sem=send_sem.at[leaving],
            recv_sem=recv_sem.at[number],
            device_id=device,
            device_id_type=MESH,
        )

    def send(leaving, number, src, dst, device):
        remote(leaving, number, src, dst, device).start()

    def arrived(number, ref):
        remote(0, number, ref, ref, pair).wait_recv()

    def left_here(leaving, ref):
        remote(leaving, 0, ref, ref, pair).wait_send()

    def pieces(count, body):
        def step(j, carry):
            body(j)
            return carry

        lax.fori_loop(0, count, step, 0)

    columns = (1 - zc, zc)
    both = (0, 1)
    top, bottom = pl.ds(0, HALF), pl.ds(HALF, HALF)
    halves = (top, bottom)
    rest = pl.ds(KEEP, ROWS - KEEP)
    kept = (top, pl.ds(HALF, KEEP - HALF))

    def slot(dy, i):
        return 2 * dy + columns[i] - zc - 1

    def quarter(block, q):
        return xg.at[rows_at(block * ROWS + q * QUARTER, QUARTER, QUARTER)]

    def to_right(number, block, q):
        send(O_AG, AGR + number, quarter(block, q), quarter(block, q), right)

    def to_left(number, block, q):
        send(O_AG, AGL + number, quarter(block, q), quarter(block, q), left)

    own = (x * ROWS, x * ROWS + HALF)
    first = (x_left * ROWS, x_right * ROWS + HALF)
    second = (
        jnp.where(x == 1, x_left * ROWS + HALF, x_opp * ROWS),
        jnp.where(x == 2, x_opp * ROWS + HALF, x_right * ROWS),
    )
    third = (
        jnp.where(x == 1, x_opp * ROWS, x_left * ROWS + HALF),
        jnp.where(x == 2, x_right * ROWS, x_opp * ROWS + HALF),
    )

    for n, q in enumerate(order):
        load_x[n].wait()

        def normalize_rows(j):
            r = rows_at(q * QUARTER + j * 16, 16, 16)
            values = xv[r, :].astype(F32)
            inv = lax.rsqrt(jnp.mean(values * values, axis=-1, keepdims=True) + 1e-05)
            xg[rows_at(x * ROWS + q * QUARTER + j * 16, 16, 16), :] = (values * inv).astype(BF16)

        pieces(QUARTER // 16, normalize_rows)
        if n == 0:
            pl.semaphore_wait(barrier, 7)

        def out_quarter():
            if q < 2:
                to_right(q, x, q)
            else:
                to_left(q - 2, x, q)

        pl.when(core == 1)(out_quarter)

    @pl.when(y == 0)
    def _():
        for i in both:
            for h in both:
                remote(O_H, H02 + 2 * i + h, hist_hbm.at[slot(2, i), kept[h]], b02.at[i, kept[h]], up).start()
            remote(O_H, H02B + i, hist_hbm.at[slot(2, i), rest], b02b.at[i], down).start()
        remote(O_H + 2, H01Z, hist_hbm.at[slot(1, 0)], z01, pair).start()

    @pl.when(y == 1)
    def _():
        for n, (i, row, count) in enumerate(FAR):
            r = pl.ds(row, count)
            remote(O_H, H13 + n, hist_hbm.at[slot(2, i), r], b13.at[i, r], down).start()
        for i in both:
            remote(O_H + 1, H12B + i, hist_hbm.at[slot(1, i), rest], b12b.at[i], up).start()

    @pl.when(y == 2)
    def _():
        for i in both:
            for h in both:
                remote(O_H, H23 + 2 * i + h, hist_hbm.at[slot(1, i), halves[h]], b23.at[i, halves[h]], up).start()

    @pl.when((y < 2) & (zc == 0))
    def _():
        for h in both:
            remote(O_HZ, HZ + h, hist_hbm.at[0, halves[h]], zr.at[halves[h]], pair).start()

    load_kv = [
        load(5, wk_hbm, wqkv.at[:, pl.ds(QW, 128)]),
        load(6, wv_hbm, wqkv.at[:, pl.ds(QW + 128, 128)]),
    ]
    load_q = load(4, wq_hbm, wqkv.at[:, pl.ds(0, QW)])
    load_mix = load(7, mix_hbm, mix)
    far = jnp.where(y == 0, 3, 1)
    load_h = [load(i, hist_hbm.at[slot(far, i)], hl.at[i]) for i in both]
    load_hm = load(2, hist_hbm.at[jnp.where(y == 0, 1, 0)], hm)
    load_wo = load(3, wo_hbm, wo)

    @pl.when(core == 0)
    def _():
        for copy in load_kv:
            copy.wait()
        to_right(0, x, 0)
        to_left(0, x, 2)
        to_right(1, x, 1)
        to_left(1, x, 3)

    @pl.when(x == 0)
    def _():
        to_right(2, x, 2)
        to_right(2, x, 3)

    @pl.when(x != 3)
    def _():
        to_left(2, x, 0)
        to_left(2, x, 1)

    def weight(y_dst, c, y_src):
        return mix[2 * (y_dst - y_src) + c - zc, y_dst * 8 + c * 4 + lax.rem(s, 4)]

    def project(group):
        r0, r1 = (rows_at(start, HALF, HALF) for start in group)

        def tile(j):
            cols = rows_at(j * 256, 256, 256)
            tokens = jnp.concatenate([xg[r0, :], xg[r1, :]], axis=0)
            out = jnp.dot(tokens, wqkv[:, cols], preferred_element_type=F32).astype(BF16)
            qkv[r0, cols] = out[:HALF]
            qkv[r1, cols] = out[HALF:]

        pieces(4, tile)
        low = lax.broadcasted_iota(jnp.int32, (HALF, 128), 1) < HEAD_DIM
        for r in (r0, r1):
            keys = qkv[r, pl.ds(QW, 128)].astype(F32)
            turned = pltpu.roll(keys, HEAD_DIM, 1)
            kc[0, r, :] = jnp.where(low, keys, turned).astype(BF16)
            kc[1, r, :] = jnp.where(low, turned, keys).astype(BF16)
            vs[r, :] = qkv[r, pl.ds(QW + 128, 128)]

    exponent_scale = math.log2(math.e) / math.sqrt(HEAD_DIM)

    def attend(group):
        r0, r1 = (rows_at(start, HALF, HALF) for start in group)
        lane = lax.broadcasted_iota(jnp.int32, (SEQ, 2 * ROWS), 1)
        lane = jnp.where(lane < ROWS, lane, lane - ROWS)
        query = lane + jnp.where(lane < HALF, group[0], group[1] - HALF)
        seen = query >= lax.broadcasted_iota(jnp.int32, (SEQ, 2 * ROWS), 0)
        low = lax.broadcasted_iota(jnp.int32, (ROWS, 128), 1) < HEAD_DIM
        turned_values = vs[...].astype(F32).T.astype(BF16)
        vt[0] = turned_values[:HEAD_DIM]
        vt[1] = turned_values[HEAD_DIM:]

        def some_pairs(j):
            for k in range(PAIR_UNROLL):
                p = PAIR_UNROLL * j + k
                g = p // (PAIRS // 2)
                cols = rows_at(p * 128, 128, 128)
                q = jnp.concatenate([qkv[r0, cols], qkv[r1, cols]], axis=0)
                zero = jnp.zeros_like(q)
                apart = jnp.concatenate([jnp.where(low, q, zero), jnp.where(low, zero, q)], axis=0)
                scores = lax.dot_general(kc[g], apart, (((1,), (1,)), ((), ())), preferred_element_type=F32)
                scores = jnp.where(seen, scores, -1e30)
                high = jnp.max(scores, axis=0, keepdims=True)
                e = jnp.exp2((scores - high) * exponent_scale)
                total = jnp.sum(e, axis=0, keepdims=True)
                probs = (e * (1.0 / total)).astype(BF16)
                out = jnp.dot(vt[g], probs, preferred_element_type=F32)
                heads[:, cols] = jnp.concatenate([out[:, :ROWS], out[:, ROWS:]], axis=0).T.astype(BF16)

        pieces(PAIRS // PAIR_UNROLL, some_pairs)

    def put_out(number):
        def tile(j):
            cols = rows_at(j * CHUNK, CHUNK, CHUNK)
            parts[number, :, cols] = jnp.dot(
                heads[...], wo[:, cols], preferred_element_type=F32
            ).astype(BF16)

        pieces(D // CHUNK, tile)

    def piece(i, ref, first_row=0):
        return ref.at[pl.ds(first_row + i * SUB, SUB)]

    def small_piece(i, ref, first_row=0):
        row, column = i // (D // WIDTH) * SUB, i % (D // WIDTH) * WIDTH
        return ref.at[pl.ds(first_row + row, SUB), pl.ds(column, WIDTH)]

    def send_parts(number, to_left_kind, to_right_kind):
        for i in range(N_P):
            send(
                O_XS,
                XS + jnp.where(to_left_kind == 0, i, 2 * N_P),
                piece(i, parts.at[number]),
                piece(i, xbuf.at[to_left_kind]),
                left,
            )
            send(
                O_XS,
                XS + jnp.where(to_right_kind == 1, N_P + i, 2 * N_P + 1),
                piece(i, parts.at[number], HALF),
                piece(i, xbuf.at[to_right_kind]),
                right,
            )

    kc[...] = jnp.zeros(kc.shape, BF16)
    vs[...] = jnp.zeros(vs.shape, BF16)
    @pl.when(core == 1)
    def _():
        for copy in load_kv:
            copy.wait()

    load_q.wait()
    project(own)

    load_mix.wait()
    for copy in load_h:
        copy.wait()
    load_hm.wait()

    def merge(count, dst, theirs, mine_weight, mine):
        def rows(j):
            r = rows_at(j * 16, 16, 16)
            dst[r, :] = (theirs * dst[r, :].astype(F32) + mine_weight * mine[r, :].astype(F32)).astype(BF16)

        pieces(count // 16, rows)

    def far_sum(n):
        i, row, count = FAR[n]
        r = pl.ds(row, count)
        arrived(H13 + n, b13.at[i, r])
        merge(count, b13.at[i, r], weight(3, columns[i], 1), weight(3, columns[i], 0), hl.at[i, r])
        remote(O_H + 1, H03 + n, b13.at[i, r], b03.at[i, r], down).start()

    for k in range(2):
        arrived(AGR + k, quarter(x_left, k))
        to_right(3, x_left, k)
        arrived(AGL + k, quarter(x_right, 2 + k))
        to_left(3, x_right, 2 + k)
        if k == 0:

            @pl.when(y == 0)
            def _():
                far_sum(0)

    @pl.when(x != 0)
    def _():
        to_right(2, x, 2)
        to_right(2, x, 3)

    @pl.when(x == 3)
    def _():
        to_left(2, x, 0)
        to_left(2, x, 1)

    def near_sum(i, h):
        n, rows = 2 * i + h, b02.at[i, kept[h]]
        arrived(H02 + n, rows)
        merge(
            (HALF, KEEP - HALF)[h], rows, weight(2, columns[i], 0), weight(2, columns[i], 1), hl.at[i, kept[h]]
        )
        remote(O_H + 1, H12 + n, rows, b12.at[i, kept[h]], up).start()

    def column_sum(i, h, add):
        c = columns[i]

        @pl.when(y == 2)
        def _():
            arrived(H12 + 2 * i + h, b12.at[i, kept[h]])

            def upper(j):
                r = rows_at(h * HALF + j * 16, 16, 16)
                add(r, b12[i, r, :].astype(F32))

            pieces((HALF, KEEP - HALF)[h] // 16, upper)
            if h == 1:
                arrived(H12B + i, b12b.at[i])
                arrived(H02C + i, b02c.at[i])
                one, two = weight(2, c, 1), weight(2, c, 0)

                def lower(j):
                    r = rows_at(j * 16, 16, 16)
                    add(
                        rows_at(KEEP + j * 16, 16, 16),
                        one * b12b[i, r, :].astype(F32) + two * b02c[i, r, :].astype(F32),
                    )

                pieces((ROWS - KEEP) // 16, lower)

        @pl.when(y == 3)
        def _():
            for n, (block, row, count) in enumerate(FAR):
                if block == i and row // HALF == h:
                    arrived(H03 + n, b03.at[i, pl.ds(row, count)])
            arrived(H23 + 2 * i + h, b23.at[i, halves[h]])
            one = weight(3, c, 2)

            def every(j):
                r = rows_at(h * HALF + j * 16, 16, 16)
                add(r, b03[i, r, :].astype(F32) + one * b23[i, r, :].astype(F32))

            pieces(HALF // 16, every)

    nearest_pair = jnp.where(zc == 0, mix[1, jnp.minimum(s + 4, 31)], F32(0.0))

    def for_pair(r, value):
        zs[r, :] = (value + nearest_pair * hm[r, :].astype(F32)).astype(BF16)

    def to_pair(h):
        column_sum(0, h, for_pair)

        @pl.when(y >= 2)
        def _():
            remote(O_HZ, HZ + h, zs.at[halves[h]], zr.at[halves[h]], pair).start()

    @pl.when(y == 0)
    def _():
        far_sum(1)

    @pl.when(y == 3)
    def _():
        for i in both:
            arrived(H02B + i, b02b.at[i])
            remote(O_H, H02C + i, b02b.at[i], b02c.at[i], down).start()

    @pl.when(y == 1)
    def _():
        near_sum(0, 0)

    project(first)

    def group_arrived(from_left, from_right):
        arrived(AGR + from_left, xg.at[top])
        arrived(AGL + from_right, xg.at[top])

    @pl.when(y == 1)
    def _():
        near_sum(0, 1)

    @pl.when(y == 0)
    def _():
        far_sum(2)

    left_2 = jnp.where(x == 1, 2, 3)
    right_2 = jnp.where(x == 2, 3, 2)
    group_arrived(left_2, right_2)
    project(second)
    to_pair(0)

    @pl.when(y == 0)
    def _():
        arrived(H01Z, z01)
        for h in both:
            merge(HALF, z01.at[halves[h]], mix[2 + zc - (1 - zc), s + 8], weight(1, zc, 0), hm.at[halves[h]])
            remote(O_H + 2, H01 + h, z01.at[halves[h]], b01.at[halves[h]], up).start()

    load_wo.wait()
    attend(second)
    put_out(2)
    left_kind = jnp.where(x == 1, 2, 0)
    right_kind = jnp.where(x == 2, 1, 3)
    send_parts(2, left_kind, right_kind)

    @pl.when(y == 0)
    def _():
        far_sum(3)

    @pl.when(y == 1)
    def _():
        near_sum(1, 0)

    group_arrived(5 - left_2, 5 - right_2)
    project(third)
    to_pair(1)

    @pl.when(y == 1)
    def _():
        near_sum(1, 1)

    attend(third)
    put_out(3)
    send_parts(3, 2 - left_kind, 4 - right_kind)

    attend(own)

    @pl.when(y == 0)
    def _():
        far_sum(4)

    put_out(0)
    attend(first)
    put_out(1)

    for i in range(N_T):
        row, column = i // (D // WIDTH) * SUB, i % (D // WIDTH) * WIDTH
        cols = pl.ds(column, WIDTH)
        for side in both:
            r, rr = pl.ds(row, SUB), pl.ds(side * HALF + row, SUB)
            if column == 0:
                arrived(XS + side * N_P + row // SUB, piece(row // SUB, xbuf.at[side]))
            parts[1, rr, cols] = (
                parts[1, rr, cols].astype(F32) + xbuf[side, r, cols].astype(F32)
            ).astype(BF16)
            send(
                O_XT,
                XT + side * N_T + i,
                small_piece(i, parts.at[1], side * HALF),
                small_piece(i, xtail.at[side]),
                (left, right)[side],
            )

    def with_pair(r, value):
        hs[r, :] = value + zr[r, :].astype(F32)

    @pl.when((y >= 2) | (zc == 1))
    def _():
        for h in both:
            arrived(HZ + h, zr.at[halves[h]])

    nearest = mix[1, s]

    def history_sum(h):
        column_sum(1, h, with_pair)

        def every_row(body):
            pieces(HALF // 16, lambda j: body(rows_at(h * HALF + j * 16, 16, 16)))

        @pl.when(y == 0)
        def _():
            def nothing(r):
                hs[r, :] = jnp.zeros((16, D), F32)

            every_row(nothing)

        @pl.when(y == 1)
        def _():
            arrived(H01 + h, b01.at[halves[h]])

            def from_row_0(r):
                hs[r, :] = b01[r, :].astype(F32)

            every_row(from_row_0)

        @pl.when((y < 2) & (zc == 1))
        def _():
            def from_pair(r):
                hs[r, :] = hs[r, :] + nearest * zr[r, :].astype(F32)

            every_row(from_pair)

    history_sum(0)
    arrived(XS + 2 * N_P, xbuf.at[2])
    arrived(XS + 2 * N_P + 1, xbuf.at[3])
    own_weight = mix[0, s]
    tail = [(i, side) for i in range(2, N_T) for side in both]
    tail = [(0, 0), (1, 0), None, (0, 1), (1, 1)] + tail
    for step in tail:
        if step is None:
            history_sum(1)
            continue
        i, side = step
        row, column = i // (D // WIDTH) * SUB, i % (D // WIDTH) * WIDTH
        r, rr = pl.ds(row, SUB), pl.ds(side * HALF + row, SUB)
        arrived(XT + side * N_T + i, small_piece(i, xtail.at[side]))

        def mix_columns(j):
            cols = rows_at(column + j * 1024, 1024, 1024)
            total = (
                parts[0, rr, cols].astype(F32)
                + xtail[side, r, cols].astype(F32)
                + xbuf[3 - side, r, cols].astype(F32)
            )
            block_out = (xv[rr, cols].astype(F32) + total).astype(BF16)
            stage[rr, cols] = (own_weight * block_out.astype(F32) + hs[rr, cols]).astype(BF16)

        pieces(WIDTH // 1024, mix_columns)
        send(O_FS, FS, small_piece(i, stage, side * HALF), small_piece(i, out_ref, side * HALF), following)

    def many(rows):
        return xg.at[pl.ds(0, rows)]

    left_here(O_AG, many(3 * ROWS))
    left_here(O_XS, many(2 * ROWS))

    @pl.when(y < 3)
    def _():
        left_here(O_H, many(2 * ROWS))

    @pl.when(y == 3)
    def _():
        left_here(O_H, many(2 * (ROWS - KEEP)))

    @pl.when(y < 2)
    def _():
        left_here(O_H + 1, many(2 * ROWS))

    @pl.when(y == 0)
    def _():
        left_here(O_H + 2, many(2 * ROWS))

    @pl.when((y >= 2) | (zc == 0))
    def _():
        left_here(O_HZ, many(ROWS))

    left_here(O_XT, many(ROWS))
    left_here(O_FS, stage)
    arrived(FS, out_ref)


def on_device(section_input, history, query_weight, key_weight, value_weight, output_weight, mix_weights):
    anywhere = pl.BlockSpec(memory_space=pl.ANY)
    block = (ROWS, D)
    out = pl.pallas_call(
        whole_tick,
        out_shape=pltpu.VMEM(block, BF16),
        in_specs=[anywhere] * 7,
        out_specs=pl.BlockSpec(memory_space=pltpu.VMEM),
        scratch_shapes=[
            pltpu.SMEM((8, 32), F32),
            pltpu.VMEM(block, BF16),
            pltpu.VMEM((SEQ, D), BF16),
            pltpu.VMEM((D, QW + 256), BF16),
            pltpu.VMEM((QW, D), BF16),
            pltpu.VMEM((SEQ, QW + 256), BF16),
            pltpu.VMEM((2, SEQ, 128), BF16),
            pltpu.VMEM((2, HEAD_DIM, SEQ), BF16),
            pltpu.VMEM((SEQ, 128), BF16),
            pltpu.VMEM((ROWS, QW), BF16),
            pltpu.VMEM((4, ROWS, D), BF16),
            pltpu.VMEM((4, HALF, D), BF16),
            pltpu.VMEM((2, HALF, D), BF16),
            pltpu.VMEM((2, KEEP, D), BF16),
            pltpu.VMEM((2, ROWS - KEEP, D), BF16),
            pltpu.VMEM((2, ROWS - KEEP, D), BF16),
            pltpu.VMEM(block, BF16),
            pltpu.VMEM((2, ROWS, D), BF16),
            pltpu.VMEM((2, ROWS, D), BF16),
            pltpu.VMEM((2, ROWS - KEEP, D), BF16),
            pltpu.VMEM((2, KEEP, D), BF16),
            pltpu.VMEM((2, ROWS, D), BF16),
            pltpu.VMEM(block, BF16),
            pltpu.VMEM(block, BF16),
            pltpu.VMEM(block, BF16),
            pltpu.VMEM((2, ROWS, D), BF16),
            pltpu.VMEM(block, BF16),
            pltpu.VMEM(block, F32),
            pltpu.VMEM(block, BF16),
            pltpu.SemaphoreType.DMA((N_LEAVING,)),
            pltpu.SemaphoreType.DMA((N_ARRIVALS,)),
            pltpu.SemaphoreType.DMA((N_LOADS,)),
        ],
        compiler_params=pltpu.CompilerParams(
            collective_id=0, has_side_effects=True, vmem_limit_bytes=60_000_000
        ),
        name="whole_tick",
    )(
        section_input[0], history[0], query_weight[0], key_weight[0], value_weight[0], output_weight[0],
        mix_weights.T,
    )
    return out[None]


def solution(mesh):
    placed = (
        P("section", "tensor", None),
        P("section", None, "tensor", None),
        P("section", None, "tensor"),
        P("section", None, "tensor"),
        P("section", None, "tensor"),
        P("section", "tensor", None),
        P(),
    )
    return jax.shard_map(
        on_device,
        mesh=mesh,
        in_specs=placed,
        out_specs=P("section", "tensor", None),
        check_vma=False,
    )
```

```python
import math

import jax
import jax.numpy as jnp
from jax import lax
from jax.experimental import pallas as pl
from jax.experimental.pallas import tpu as pltpu
from jax.sharding import PartitionSpec as P

HEAD_DIM = 64
MESH = pl.DeviceIdType.MESH
F32 = jnp.float32
BF16 = jnp.bfloat16
ROWS = 128
HALF = 64
D = 4096
SEQ = 512
QW = 768
PAIRS = QW // 128
PAIR_UNROLL = 2
KEEP = 96
QUARTER = 32
FAR = ((0, 0, 32), (0, 32, 32), (0, HALF, HALF), (1, 0, HALF), (1, HALF, 32), (1, 96, 32))
LAST = ((0, HALF), (HALF, 32), (96, 32))
CHUNK = 1024
SUB = 16
N_P = HALF // SUB
TAIL = ((0, 0, D // 2), (0, D // 2, D // 2), (16, 0, D), (32, 0, D), (48, 0, D // 2), (48, D // 2, D // 2))
N_T = len(TAIL)
AGR, AGL = 0, 4
XS = 8
XT = XS + 2 * N_P + 2
FS = XT + 2 * N_T
HZ = FS + 1
H = HZ + 2
H13, H01Z = H, H + 6
H02, H01 = H, H + 4
H12, H12B, H02C = H, H + 4, H + 6
H03, H23, H02B = H, H + 6, H + 10
N_ARRIVALS = H + 12
O_AG, O_XS, O_XT, O_FS, O_HZ, O_H = 0, 1, 2, 3, 4, 5
N_LEAVING = O_H + 3
N_LOADS = 8


def rows_at(start, size, step):
    return pl.ds(pl.multiple_of(start, step), size)


def whole_tick(
    x_hbm, hist_hbm, wq_hbm, wk_hbm, wv_hbm, wo_hbm, mix_hbm, out_ref,
    mix, xv, xg, wqkv, wo, qkv, kc, vt, vs, heads, parts, xbuf, xtail,
    b02, b02b, b02c, b01, b13, b03, b12b, b12, b23, z01, zr, zs, hl, hm, hs, stage,
    send_sem, recv_sem, load_sem,
):
    def load(number, src, dst):
        copy = pltpu.make_async_copy(src, dst, load_sem.at[number])
        copy.start()
        return copy

    order = (0, 2, 1, 3)
    load_x = []
    for n, q in enumerate(order):
        r = pl.ds(q * QUARTER, QUARTER)
        load_x.append(load(n, x_hbm.at[r], xv.at[r]))

    s = lax.axis_index("section")
    x = lax.axis_index("tensor")
    core = lax.rem(s, 2)
    y = s // 8
    zc = lax.rem(s // 4, 2)
    x_right, x_left, x_opp = lax.rem(x + 1, 4), lax.rem(x + 3, 4), lax.rem(x + 2, 4)
    right, left = (s, x_right), (s, x_left)
    up, down = (lax.rem(s + 8, 32), x), (lax.rem(s + 24, 32), x)
    pair = (s + 4 - 8 * zc, x)
    following, preceding = (lax.rem(s + 1, 32), x), (lax.rem(s + 31, 32), x)

    barrier = pltpu.get_barrier_semaphore()
    for other in (right, left, up, down, pair, preceding):
        pl.semaphore_signal(barrier, inc=1, device_id=other, device_id_type=MESH)

    def remote(leaving, number, src, dst, device):
        return pltpu.make_async_remote_copy(
            src_ref=src,
            dst_ref=dst,
            send_sem=send_sem.at[leaving],
            recv_sem=recv_sem.at[number],
            device_id=device,
            device_id_type=MESH,
        )

    def send(leaving, number, src, dst, device):
        remote(leaving, number, src, dst, device).start()

    def arrived(number, ref):
        remote(0, number, ref, ref, pair).wait_recv()

    def left_here(leaving, ref):
        remote(leaving, 0, ref, ref, pair).wait_send()

    def pieces(count, body):
        def step(j, carry):
            body(j)
            return carry

        lax.fori_loop(0, count, step, 0)

    columns = (1 - zc, zc)
    both = (0, 1)
    top, bottom = pl.ds(0, HALF), pl.ds(HALF, HALF)
    halves = (top, bottom)
    rest = pl.ds(KEEP, ROWS - KEEP)
    kept = (top, pl.ds(HALF, KEEP - HALF))

    def slot(dy, i):
        return 2 * dy + columns[i] - zc - 1

    def quarter(block, q):
        return xg.at[rows_at(block * ROWS + q * QUARTER, QUARTER, QUARTER)]

    def to_right(number, block, q):
        send(O_AG, AGR + number, quarter(block, q), quarter(block, q), right)

    def to_left(number, block, q):
        send(O_AG, AGL + number, quarter(block, q), quarter(block, q), left)

    own = (x * ROWS, x * ROWS + HALF)
    first = (x_left * ROWS, x_right * ROWS + HALF)
    second = (
        jnp.where(x == 1, x_left * ROWS + HALF, x_opp * ROWS),
        jnp.where(x == 2, x_opp * ROWS + HALF, x_right * ROWS),
    )
    third = (
        jnp.where(x == 1, x_opp * ROWS, x_left * ROWS + HALF),
        jnp.where(x == 2, x_right * ROWS, x_opp * ROWS + HALF),
    )

    for n, q in enumerate(order):
        load_x[n].wait()

        def normalize_rows(j):
            r = rows_at(q * QUARTER + j * 16, 16, 16)
            values = xv[r, :].astype(F32)
            inv = lax.rsqrt(jnp.mean(values * values, axis=-1, keepdims=True) + 1e-05)
            xg[rows_at(x * ROWS + q * QUARTER + j * 16, 16, 16), :] = (values * inv).astype(BF16)

        pieces(QUARTER // 16, normalize_rows)
        if n == 0:
            pl.semaphore_wait(barrier, 6)

        def out_quarter():
            if q < 2:
                to_right(q, x, q)
            else:
                to_left(q - 2, x, q)

        pl.when(core == 1)(out_quarter)

    def stored_history():
        @pl.when(y == 0)
        def _():
            for i in both:
                for h in both:
                    remote(O_H, H02 + 2 * i + h, hist_hbm.at[slot(2, i), kept[h]], b02.at[i, kept[h]], up).start()
                remote(O_H, H02B + i, hist_hbm.at[slot(2, i), rest], b02b.at[i], down).start()
            remote(O_H + 2, H01Z, hist_hbm.at[slot(1, 0)], z01, pair).start()

        @pl.when(y == 1)
        def _():
            for n, (i, row, count) in enumerate(FAR):
                r = pl.ds(row, count)
                remote(O_H, H13 + n, hist_hbm.at[slot(2, i), r], b13.at[i, r], down).start()
            for i in both:
                remote(O_H + 1, H12B + i, hist_hbm.at[slot(1, i), rest], b12b.at[i], up).start()

        @pl.when(y == 2)
        def _():
            for i in both:
                for h in both:
                    remote(O_H, H23 + 2 * i + h, hist_hbm.at[slot(1, i), halves[h]], b23.at[i, halves[h]], up).start()

        @pl.when((y < 2) & (zc == 0))
        def _():
            for h in both:
                remote(O_HZ, HZ + h, hist_hbm.at[0, halves[h]], zr.at[halves[h]], pair).start()

    pl.when(core == 1)(stored_history)

    load_kv = [
        load(5, wk_hbm, wqkv.at[:, pl.ds(QW, 128)]),
        load(6, wv_hbm, wqkv.at[:, pl.ds(QW + 128, 128)]),
    ]
    load_q = load(4, wq_hbm, wqkv.at[:, pl.ds(0, QW)])
    load_mix = load(7, mix_hbm, mix)
    far = jnp.where(y == 0, 3, 1)
    load_h = [load(i, hist_hbm.at[slot(far, i)], hl.at[i]) for i in both]
    load_hm = load(2, hist_hbm.at[jnp.where(y == 0, 1, 0)], hm)
    load_wo = load(3, wo_hbm, wo)

    yields = (core == 0) & (lax.rem(s // 2, 4) == 3)

    def weights_loaded():
        for copy in load_kv:
            copy.wait()
        load_q.wait()

    pl.when(yields)(weights_loaded)

    @pl.when(core == 0)
    def _():
        stored_history()
        to_right(0, x, 0)
        to_left(0, x, 2)
        to_right(1, x, 1)
        to_left(1, x, 3)

    @pl.when(x == 0)
    def _():
        to_right(2, x, 2)
        to_right(2, x, 3)

    @pl.when(x != 3)
    def _():
        to_left(2, x, 0)
        to_left(2, x, 1)

    def weight(y_dst, c, y_src):
        return mix[2 * (y_dst - y_src) + c - zc, y_dst * 8 + c * 4 + lax.rem(s, 4)]

    def project(group):
        r0, r1 = (rows_at(start, HALF, HALF) for start in group)

        def tile(j):
            cols = rows_at(j * 256, 256, 256)
            tokens = jnp.concatenate([xg[r0, :], xg[r1, :]], axis=0)
            out = jnp.dot(tokens, wqkv[:, cols], preferred_element_type=F32).astype(BF16)
            qkv[r0, cols] = out[:HALF]
            qkv[r1, cols] = out[HALF:]

        pieces(4, tile)
        low = lax.broadcasted_iota(jnp.int32, (HALF, 128), 1) < HEAD_DIM
        for r in (r0, r1):
            keys = qkv[r, pl.ds(QW, 128)].astype(F32)
            turned = pltpu.roll(keys, HEAD_DIM, 1)
            kc[0, r, :] = jnp.where(low, keys, turned).astype(BF16)
            kc[1, r, :] = jnp.where(low, turned, keys).astype(BF16)
            vs[r, :] = qkv[r, pl.ds(QW + 128, 128)]

    exponent_scale = math.log2(math.e) / math.sqrt(HEAD_DIM)

    def attend(group):
        r0, r1 = (rows_at(start, HALF, HALF) for start in group)
        lane = lax.broadcasted_iota(jnp.int32, (SEQ, 2 * ROWS), 1)
        lane = jnp.where(lane < ROWS, lane, lane - ROWS)
        query = lane + jnp.where(lane < HALF, group[0], group[1] - HALF)
        seen = query >= lax.broadcasted_iota(jnp.int32, (SEQ, 2 * ROWS), 0)
        low = lax.broadcasted_iota(jnp.int32, (ROWS, 128), 1) < HEAD_DIM
        turned_values = vs[...].astype(F32).T.astype(BF16)
        vt[0] = turned_values[:HEAD_DIM]
        vt[1] = turned_values[HEAD_DIM:]

        def some_pairs(j):
            for k in range(PAIR_UNROLL):
                p = PAIR_UNROLL * j + k
                g = p // (PAIRS // 2)
                cols = rows_at(p * 128, 128, 128)
                q = jnp.concatenate([qkv[r0, cols], qkv[r1, cols]], axis=0)
                zero = jnp.zeros_like(q)
                apart = jnp.concatenate([jnp.where(low, q, zero), jnp.where(low, zero, q)], axis=0)
                scores = lax.dot_general(kc[g], apart, (((1,), (1,)), ((), ())), preferred_element_type=F32)
                scores = jnp.where(seen, scores, -1e30)
                high = jnp.max(scores, axis=0, keepdims=True)
                e = jnp.exp2((scores - high) * exponent_scale)
                total = jnp.sum(e, axis=0, keepdims=True)
                probs = (e * (1.0 / total)).astype(BF16)
                out = jnp.dot(vt[g], probs, preferred_element_type=F32)
                heads[:, cols] = jnp.concatenate([out[:, :ROWS], out[:, ROWS:]], axis=0).T.astype(BF16)

        pieces(PAIRS // PAIR_UNROLL, some_pairs)

    def put_out(number):
        def tile(j):
            cols = rows_at(j * CHUNK, CHUNK, CHUNK)
            parts[number, :, cols] = jnp.dot(
                heads[...], wo[:, cols], preferred_element_type=F32
            ).astype(BF16)

        pieces(D // CHUNK, tile)

    def piece(i, ref, first_row=0):
        return ref.at[pl.ds(first_row + i * SUB, SUB)]

    def small_piece(i, ref, first_row=0):
        row, column, width = TAIL[i]
        return ref.at[pl.ds(first_row + row, SUB), pl.ds(column, width)]

    def send_parts(number, to_left_kind, to_right_kind):
        for i in range(N_P):
            send(
                O_XS,
                XS + jnp.where(to_left_kind == 0, i, 2 * N_P),
                piece(i, parts.at[number]),
                piece(i, xbuf.at[to_left_kind]),
                left,
            )
            send(
                O_XS,
                XS + jnp.where(to_right_kind == 1, N_P + i, 2 * N_P + 1),
                piece(i, parts.at[number], HALF),
                piece(i, xbuf.at[to_right_kind]),
                right,
            )

    kc[...] = jnp.zeros(kc.shape, BF16)
    vs[...] = jnp.zeros(vs.shape, BF16)
    pl.when(jnp.logical_not(yields))(weights_loaded)
    project(own)

    load_mix.wait()
    for copy in load_h:
        copy.wait()
    load_hm.wait()

    def merge(count, dst, theirs, mine_weight, mine):
        def rows(j):
            r = rows_at(j * 16, 16, 16)
            dst[r, :] = (theirs * dst[r, :].astype(F32) + mine_weight * mine[r, :].astype(F32)).astype(BF16)

        pieces(count // 16, rows)

    def far_sum(n):
        i, row, count = FAR[n]
        r = pl.ds(row, count)
        arrived(H13 + n, b13.at[i, r])
        merge(count, b13.at[i, r], weight(3, columns[i], 1), weight(3, columns[i], 0), hl.at[i, r])
        remote(O_H + 1, H03 + n, b13.at[i, r], b03.at[i, r], down).start()

    for k in range(2):
        arrived(AGR + k, quarter(x_left, k))
        to_right(3, x_left, k)
        arrived(AGL + k, quarter(x_right, 2 + k))
        to_left(3, x_right, 2 + k)
        if k == 0:

            @pl.when(y == 0)
            def _():
                far_sum(0)

    @pl.when(x != 0)
    def _():
        to_right(2, x, 2)
        to_right(2, x, 3)

    @pl.when(x == 3)
    def _():
        to_left(2, x, 0)
        to_left(2, x, 1)

    def near_sum(i, h):
        n, rows = 2 * i + h, b02.at[i, kept[h]]
        arrived(H02 + n, rows)
        merge(
            (HALF, KEEP - HALF)[h], rows, weight(2, columns[i], 0), weight(2, columns[i], 1), hl.at[i, kept[h]]
        )
        remote(O_H + 1, H12 + n, rows, b12.at[i, kept[h]], up).start()

    def column_sum(i, row, count, add):
        c = columns[i]

        @pl.when(y == 2)
        def _():
            if row <= HALF:
                h = row // HALF
                arrived(H12 + 2 * i + h, b12.at[i, kept[h]])

                def upper(j):
                    r = rows_at(row + j * 16, 16, 16)
                    add(r, b12[i, r, :].astype(F32))

                pieces((HALF, KEEP - HALF)[h] // 16, upper)
            if row + count == ROWS:
                arrived(H12B + i, b12b.at[i])
                arrived(H02C + i, b02c.at[i])
                one, two = weight(2, c, 1), weight(2, c, 0)

                def lower(j):
                    r = rows_at(j * 16, 16, 16)
                    add(
                        rows_at(KEEP + j * 16, 16, 16),
                        one * b12b[i, r, :].astype(F32) + two * b02c[i, r, :].astype(F32),
                    )

                pieces((ROWS - KEEP) // 16, lower)

        @pl.when(y == 3)
        def _():
            for n, (block, far_row, far_count) in enumerate(FAR):
                if block == i and row <= far_row < row + count:
                    arrived(H03 + n, b03.at[i, pl.ds(far_row, far_count)])
            if row <= HALF:
                h = row // HALF
                arrived(H23 + 2 * i + h, b23.at[i, halves[h]])
            one = weight(3, c, 2)

            def every(j):
                r = rows_at(row + j * 16, 16, 16)
                add(r, b03[i, r, :].astype(F32) + one * b23[i, r, :].astype(F32))

            pieces(count // 16, every)

    nearest_pair = jnp.where(zc == 0, mix[1, jnp.minimum(s + 4, 31)], F32(0.0))

    def for_pair(r, value):
        zs[r, :] = (value + nearest_pair * hm[r, :].astype(F32)).astype(BF16)

    def to_pair(h):
        column_sum(0, h * HALF, HALF, for_pair)

        @pl.when(y >= 2)
        def _():
            remote(O_HZ, HZ + h, zs.at[halves[h]], zr.at[halves[h]], pair).start()

    @pl.when(y == 3)
    def _():
        for i in both:
            arrived(H02B + i, b02b.at[i])
            remote(O_H, H02C + i, b02b.at[i], b02c.at[i], down).start()

    @pl.when(y == 1)
    def _():
        near_sum(0, 0)

    project(first)

    @pl.when(y == 0)
    def _():
        far_sum(1)

    def group_arrived(from_left, from_right):
        arrived(AGR + from_left, xg.at[top])
        arrived(AGL + from_right, xg.at[top])

    @pl.when(y == 1)
    def _():
        near_sum(0, 1)

    left_2 = jnp.where(x == 1, 2, 3)
    right_2 = jnp.where(x == 2, 3, 2)
    group_arrived(left_2, right_2)
    project(second)

    @pl.when(y == 0)
    def _():
        far_sum(2)

    to_pair(0)

    @pl.when(y == 0)
    def _():
        arrived(H01Z, z01)
        for n, (row, count) in enumerate(LAST):
            r = pl.ds(row, count)
            merge(count, z01.at[r], mix[2 + zc - (1 - zc), s + 8], weight(1, zc, 0), hm.at[r])
            remote(O_H + 2, H01 + n, z01.at[r], b01.at[r], up).start()

    load_wo.wait()
    attend(second)
    put_out(2)
    left_kind = jnp.where(x == 1, 2, 0)
    right_kind = jnp.where(x == 2, 1, 3)
    send_parts(2, left_kind, right_kind)

    @pl.when(y == 1)
    def _():
        near_sum(1, 0)

    group_arrived(5 - left_2, 5 - right_2)
    project(third)

    @pl.when(y == 0)
    def _():
        far_sum(3)

    to_pair(1)

    @pl.when(y == 1)
    def _():
        near_sum(1, 1)

    attend(third)
    put_out(3)
    send_parts(3, 2 - left_kind, 4 - right_kind)

    @pl.when(y == 0)
    def _():
        far_sum(4)

    attend(own)

    @pl.when(y == 0)
    def _():
        far_sum(5)

    put_out(0)
    attend(first)
    put_out(1)

    for i in range(N_T):
        row, column, width = TAIL[i]
        cols = pl.ds(column, width)
        for side in both:
            r, rr = pl.ds(row, SUB), pl.ds(side * HALF + row, SUB)
            if column == 0:
                arrived(XS + side * N_P + row // SUB, piece(row // SUB, xbuf.at[side]))
            parts[1, rr, cols] = (
                parts[1, rr, cols].astype(F32) + xbuf[side, r, cols].astype(F32)
            ).astype(BF16)
            send(
                O_XT,
                XT + side * N_T + i,
                small_piece(i, parts.at[1], side * HALF),
                small_piece(i, xtail.at[side]),
                (left, right)[side],
            )

    def with_pair(r, value):
        hs[r, :] = value + zr[r, :].astype(F32)

    @pl.when((y >= 2) | (zc == 1))
    def _():
        for h in both:
            arrived(HZ + h, zr.at[halves[h]])

    nearest = mix[1, s]

    def history_sum(n):
        row, count = LAST[n]
        column_sum(1, row, count, with_pair)

        def every_row(body):
            pieces(count // 16, lambda j: body(rows_at(row + j * 16, 16, 16)))

        @pl.when(y == 0)
        def _():
            def nothing(r):
                hs[r, :] = jnp.zeros((16, D), F32)

            every_row(nothing)

        @pl.when(y == 1)
        def _():
            arrived(H01 + n, b01.at[pl.ds(row, count)])

            def from_row_0(r):
                hs[r, :] = b01[r, :].astype(F32)

            every_row(from_row_0)

        @pl.when((y < 2) & (zc == 1))
        def _():
            def from_pair(r):
                hs[r, :] = hs[r, :] + nearest * zr[r, :].astype(F32)

            every_row(from_pair)

    history_sum(0)
    arrived(XS + 2 * N_P, xbuf.at[2])
    arrived(XS + 2 * N_P + 1, xbuf.at[3])
    own_weight = mix[0, s]
    tail = [(0, 0), (1, 0), 1, (0, 1), (1, 1), (2, 0), (2, 1), 2]
    tail += [(i, side) for i in range(3, N_T) for side in both]
    for step in tail:
        if step in (1, 2):
            history_sum(step)
            continue
        i, side = step
        row, column, width = TAIL[i]
        r, rr = pl.ds(row, SUB), pl.ds(side * HALF + row, SUB)
        arrived(XT + side * N_T + i, small_piece(i, xtail.at[side]))

        def mix_columns(j):
            cols = rows_at(column + j * 1024, 1024, 1024)
            total = (
                parts[0, rr, cols].astype(F32)
                + xtail[side, r, cols].astype(F32)
                + xbuf[3 - side, r, cols].astype(F32)
            )
            block_out = (xv[rr, cols].astype(F32) + total).astype(BF16)
            stage[rr, cols] = (own_weight * block_out.astype(F32) + hs[rr, cols]).astype(BF16)

        pieces(width // 1024, mix_columns)
        send(O_FS, FS, small_piece(i, stage, side * HALF), small_piece(i, out_ref, side * HALF), following)

    def many(rows):
        return xg.at[pl.ds(0, rows)]

    left_here(O_AG, many(3 * ROWS))
    left_here(O_XS, many(2 * ROWS))

    @pl.when(y < 3)
    def _():
        left_here(O_H, many(2 * ROWS))

    @pl.when(y == 3)
    def _():
        left_here(O_H, many(2 * (ROWS - KEEP)))

    @pl.when(y < 2)
    def _():
        left_here(O_H + 1, many(2 * ROWS))

    @pl.when(y == 0)
    def _():
        left_here(O_H + 2, many(2 * ROWS))

    @pl.when((y >= 2) | (zc == 0))
    def _():
        left_here(O_HZ, many(ROWS))

    left_here(O_XT, many(ROWS))
    left_here(O_FS, stage)
    arrived(FS, out_ref)


def on_device(section_input, history, query_weight, key_weight, value_weight, output_weight, mix_weights):
    anywhere = pl.BlockSpec(memory_space=pl.ANY)
    block = (ROWS, D)
    out = pl.pallas_call(
        whole_tick,
        out_shape=pltpu.VMEM(block, BF16),
        in_specs=[anywhere] * 7,
        out_specs=pl.BlockSpec(memory_space=pltpu.VMEM),
        scratch_shapes=[
            pltpu.SMEM((8, 32), F32),
            pltpu.VMEM(block, BF16),
            pltpu.VMEM((SEQ, D), BF16),
            pltpu.VMEM((D, QW + 256), BF16),
            pltpu.VMEM((QW, D), BF16),
            pltpu.VMEM((SEQ, QW + 256), BF16),
            pltpu.VMEM((2, SEQ, 128), BF16),
            pltpu.VMEM((2, HEAD_DIM, SEQ), BF16),
            pltpu.VMEM((SEQ, 128), BF16),
            pltpu.VMEM((ROWS, QW), BF16),
            pltpu.VMEM((4, ROWS, D), BF16),
            pltpu.VMEM((4, HALF, D), BF16),
            pltpu.VMEM((2, HALF, D), BF16),
            pltpu.VMEM((2, KEEP, D), BF16),
            pltpu.VMEM((2, ROWS - KEEP, D), BF16),
            pltpu.VMEM((2, ROWS - KEEP, D), BF16),
            pltpu.VMEM(block, BF16),
            pltpu.VMEM((2, ROWS, D), BF16),
            pltpu.VMEM((2, ROWS, D), BF16),
            pltpu.VMEM((2, ROWS - KEEP, D), BF16),
            pltpu.VMEM((2, KEEP, D), BF16),
            pltpu.VMEM((2, ROWS, D), BF16),
            pltpu.VMEM(block, BF16),
            pltpu.VMEM(block, BF16),
            pltpu.VMEM(block, BF16),
            pltpu.VMEM((2, ROWS, D), BF16),
            pltpu.VMEM(block, BF16),
            pltpu.VMEM(block, F32),
            pltpu.VMEM(block, BF16),
            pltpu.SemaphoreType.DMA((N_LEAVING,)),
            pltpu.SemaphoreType.DMA((N_ARRIVALS,)),
            pltpu.SemaphoreType.DMA((N_LOADS,)),
        ],
        compiler_params=pltpu.CompilerParams(
            collective_id=0, has_side_effects=True, vmem_limit_bytes=60_000_000
        ),
        name="whole_tick",
    )(
        section_input[0], history[0], query_weight[0], key_weight[0], value_weight[0], output_weight[0],
        mix_weights.T,
    )
    return out[None]


def solution(mesh):
    placed = (
        P("section", "tensor", None),
        P("section", None, "tensor", None),
        P("section", None, "tensor"),
        P("section", None, "tensor"),
        P("section", None, "tensor"),
        P("section", "tensor", None),
        P(),
    )
    return jax.shard_map(
        on_device,
        mesh=mesh,
        in_specs=placed,
        out_specs=P("section", "tensor", None),
        check_vma=False,
    )
```

```python
import math

import jax
import jax.numpy as jnp
from jax import lax
from jax.experimental import pallas as pl
from jax.experimental.pallas import tpu as pltpu
from jax.sharding import PartitionSpec as P

HEAD_DIM = 64
MESH = pl.DeviceIdType.MESH
F32 = jnp.float32
BF16 = jnp.bfloat16
ROWS = 128
HALF = 64
D = 4096
SEQ = 512
QW = 768
PAIRS = QW // 128
PAIR_UNROLL = 2
KEEP = 96
QUARTER = 32
FAR = ((0, 0, 32), (0, 32, 32), (0, HALF, HALF), (1, 0, HALF), (1, HALF, 32), (1, 96, 32))
LAST = ((0, HALF), (HALF, 32), (96, 32))
CHUNK = 1024
SUB = 16
N_P = HALF // SUB
TAIL = ((0, 0, D // 2), (0, D // 2, D // 2), (16, 0, D), (32, 0, D), (48, 0, D // 2), (48, D // 2, D // 2))
N_T = len(TAIL)
AGR, AGL = 0, 4
XS = 8
XT = XS + 2 * N_P + 2
FS = XT + 2 * N_T
HZ = FS + 1
H = HZ + 2
H13, H01Z = H, H + 6
H02, H01 = H, H + 4
H12, H12B, H02C = H, H + 4, H + 6
H03, H23, H02B = H, H + 6, H + 10
N_ARRIVALS = H + 12
O_AG, O_XS, O_XT, O_FS, O_HZ, O_H = 0, 1, 2, 3, 4, 5
N_LEAVING = O_H + 3
N_LOADS = 8


def rows_at(start, size, step):
    return pl.ds(pl.multiple_of(start, step), size)


def whole_tick(
    x_hbm, hist_hbm, wq_hbm, wk_hbm, wv_hbm, wo_hbm, mix_hbm, out_ref,
    mix, xv, xg, wqkv, wo, qkv, kc, vt, vs, heads, parts, xbuf, xtail,
    b02, b02b, b02c, b01, b13, b03, b12b, b12, b23, z01, zr, zs, hl, hm, hs, stage,
    send_sem, recv_sem, load_sem, pair_there,
):
    def load(number, src, dst):
        copy = pltpu.make_async_copy(src, dst, load_sem.at[number])
        copy.start()
        return copy

    order = (0, 2, 1, 3)
    load_x = []
    for n, q in enumerate(order):
        r = pl.ds(q * QUARTER, QUARTER)
        load_x.append(load(n, x_hbm.at[r], xv.at[r]))

    s = lax.axis_index("section")
    x = lax.axis_index("tensor")
    core = lax.rem(s, 2)
    y = s // 8
    zc = lax.rem(s // 4, 2)
    x_right, x_left, x_opp = lax.rem(x + 1, 4), lax.rem(x + 3, 4), lax.rem(x + 2, 4)
    right, left = (s, x_right), (s, x_left)
    up, down = (lax.rem(s + 8, 32), x), (lax.rem(s + 24, 32), x)
    pair = (s + 4 - 8 * zc, x)
    following, preceding = (lax.rem(s + 1, 32), x), (lax.rem(s + 31, 32), x)

    barrier = pltpu.get_barrier_semaphore()
    for other in (right, left, up, down, preceding):
        pl.semaphore_signal(barrier, inc=1, device_id=other, device_id_type=MESH)

    @pl.when(zc == 0)
    def _():
        pl.semaphore_signal(barrier, inc=1, device_id=pair, device_id_type=MESH)

    def remote(leaving, number, src, dst, device):
        return pltpu.make_async_remote_copy(
            src_ref=src,
            dst_ref=dst,
            send_sem=send_sem.at[leaving],
            recv_sem=recv_sem.at[number],
            device_id=device,
            device_id_type=MESH,
        )

    def send(leaving, number, src, dst, device):
        remote(leaving, number, src, dst, device).start()

    def arrived(number, ref):
        remote(0, number, ref, ref, pair).wait_recv()

    def left_here(leaving, ref):
        remote(leaving, 0, ref, ref, pair).wait_send()

    def pieces(count, body):
        def step(j, carry):
            body(j)
            return carry

        lax.fori_loop(0, count, step, 0)

    columns = (1 - zc, zc)
    both = (0, 1)
    top, bottom = pl.ds(0, HALF), pl.ds(HALF, HALF)
    halves = (top, bottom)
    rest = pl.ds(KEEP, ROWS - KEEP)
    kept = (top, pl.ds(HALF, KEEP - HALF))

    def slot(dy, i):
        return 2 * dy + columns[i] - zc - 1

    def quarter(block, q):
        return xg.at[rows_at(block * ROWS + q * QUARTER, QUARTER, QUARTER)]

    def to_right(number, block, q):
        send(O_AG, AGR + number, quarter(block, q), quarter(block, q), right)

    def to_left(number, block, q):
        send(O_AG, AGL + number, quarter(block, q), quarter(block, q), left)

    own = (x * ROWS, x * ROWS + HALF)
    first = (x_left * ROWS, x_right * ROWS + HALF)
    second = (
        jnp.where(x == 1, x_left * ROWS + HALF, x_opp * ROWS),
        jnp.where(x == 2, x_opp * ROWS + HALF, x_right * ROWS),
    )
    third = (
        jnp.where(x == 1, x_opp * ROWS, x_left * ROWS + HALF),
        jnp.where(x == 2, x_right * ROWS, x_opp * ROWS + HALF),
    )

    for n, q in enumerate(order):
        load_x[n].wait()

        def normalize_rows(j):
            r = rows_at(q * QUARTER + j * 16, 16, 16)
            values = xv[r, :].astype(F32)
            inv = lax.rsqrt(jnp.mean(values * values, axis=-1, keepdims=True) + 1e-05)
            xg[rows_at(x * ROWS + q * QUARTER + j * 16, 16, 16), :] = (values * inv).astype(BF16)

        pieces(QUARTER // 16, normalize_rows)
        if n == 0:
            pl.semaphore_wait(barrier, 5 + zc)

            @pl.when(zc == 1)
            def _():
                pl.semaphore_signal(pair_there, inc=1, device_id=pair, device_id_type=MESH)

        def out_quarter():
            if q < 2:
                to_right(q, x, q)
            else:
                to_left(q - 2, x, q)

        pl.when(core == 1)(out_quarter)

    def stored_history():
        @pl.when(y == 0)
        def _():
            for i in both:
                for h in both:
                    remote(O_H, H02 + 2 * i + h, hist_hbm.at[slot(2, i), kept[h]], b02.at[i, kept[h]], up).start()
                remote(O_H, H02B + i, hist_hbm.at[slot(2, i), rest], b02b.at[i], down).start()

        @pl.when(y == 1)
        def _():
            for n, (i, row, count) in enumerate(FAR):
                r = pl.ds(row, count)
                remote(O_H, H13 + n, hist_hbm.at[slot(2, i), r], b13.at[i, r], down).start()
            for i in both:
                remote(O_H + 1, H12B + i, hist_hbm.at[slot(1, i), rest], b12b.at[i], up).start()

        @pl.when(y == 2)
        def _():
            for i in both:
                for h in both:
                    remote(O_H, H23 + 2 * i + h, hist_hbm.at[slot(1, i), halves[h]], b23.at[i, halves[h]], up).start()

    pl.when(core == 1)(stored_history)

    load_kv = [
        load(5, wk_hbm, wqkv.at[:, pl.ds(QW, 128)]),
        load(6, wv_hbm, wqkv.at[:, pl.ds(QW + 128, 128)]),
    ]
    load_q = load(4, wq_hbm, wqkv.at[:, pl.ds(0, QW)])
    load_mix = load(7, mix_hbm, mix)
    far = jnp.where(y == 0, 3, 1)
    load_h = [load(i, hist_hbm.at[slot(far, i)], hl.at[i]) for i in both]
    load_hm = load(2, hist_hbm.at[jnp.where(y == 0, 1, 0)], hm)
    load_wo = load(3, wo_hbm, wo)

    yields = (core == 0) & (lax.rem(s // 2, 4) == 3)

    def weights_loaded():
        for copy in load_kv:
            copy.wait()
        load_q.wait()

    pl.when(yields)(weights_loaded)

    @pl.when(core == 0)
    def _():
        stored_history()
        to_right(0, x, 0)
        to_left(0, x, 2)
        to_right(1, x, 1)
        to_left(1, x, 3)

    @pl.when(x == 0)
    def _():
        to_right(2, x, 2)
        to_right(2, x, 3)

    @pl.when(x != 3)
    def _():
        to_left(2, x, 0)
        to_left(2, x, 1)

    @pl.when(zc == 0)
    def _():
        pl.semaphore_wait(pair_there, 1)

    @pl.when(y == 0)
    def _():
        remote(O_H + 2, H01Z, hist_hbm.at[slot(1, 0)], z01, pair).start()

    @pl.when((y < 2) & (zc == 0))
    def _():
        for h in both:
            remote(O_HZ, HZ + h, hist_hbm.at[0, halves[h]], zr.at[halves[h]], pair).start()

    def weight(y_dst, c, y_src):
        return mix[2 * (y_dst - y_src) + c - zc, y_dst * 8 + c * 4 + lax.rem(s, 4)]

    def project(group):
        r0, r1 = (rows_at(start, HALF, HALF) for start in group)

        def tile(j):
            cols = rows_at(j * 256, 256, 256)
            tokens = jnp.concatenate([xg[r0, :], xg[r1, :]], axis=0)
            out = jnp.dot(tokens, wqkv[:, cols], preferred_element_type=F32).astype(BF16)
            qkv[r0, cols] = out[:HALF]
            qkv[r1, cols] = out[HALF:]

        pieces(4, tile)
        low = lax.broadcasted_iota(jnp.int32, (HALF, 128), 1) < HEAD_DIM
        for r in (r0, r1):
            keys = qkv[r, pl.ds(QW, 128)].astype(F32)
            turned = pltpu.roll(keys, HEAD_DIM, 1)
            kc[0, r, :] = jnp.where(low, keys, turned).astype(BF16)
            kc[1, r, :] = jnp.where(low, turned, keys).astype(BF16)
            vs[r, :] = qkv[r, pl.ds(QW + 128, 128)]

    exponent_scale = math.log2(math.e) / math.sqrt(HEAD_DIM)

    def attend(group):
        r0, r1 = (rows_at(start, HALF, HALF) for start in group)
        lane = lax.broadcasted_iota(jnp.int32, (SEQ, 2 * ROWS), 1)
        lane = jnp.where(lane < ROWS, lane, lane - ROWS)
        query = lane + jnp.where(lane < HALF, group[0], group[1] - HALF)
        seen = query >= lax.broadcasted_iota(jnp.int32, (SEQ, 2 * ROWS), 0)
        low = lax.broadcasted_iota(jnp.int32, (ROWS, 128), 1) < HEAD_DIM
        turned_values = vs[...].astype(F32).T.astype(BF16)
        vt[0] = turned_values[:HEAD_DIM]
        vt[1] = turned_values[HEAD_DIM:]

        def some_pairs(j):
            for k in range(PAIR_UNROLL):
                p = PAIR_UNROLL * j + k
                g = p // (PAIRS // 2)
                cols = rows_at(p * 128, 128, 128)
                q = jnp.concatenate([qkv[r0, cols], qkv[r1, cols]], axis=0)
                zero = jnp.zeros_like(q)
                apart = jnp.concatenate([jnp.where(low, q, zero), jnp.where(low, zero, q)], axis=0)
                scores = lax.dot_general(kc[g], apart, (((1,), (1,)), ((), ())), preferred_element_type=F32)
                scores = jnp.where(seen, scores, -1e30)
                high = jnp.max(scores, axis=0, keepdims=True)
                e = jnp.exp2((scores - high) * exponent_scale)
                total = jnp.sum(e, axis=0, keepdims=True)
                probs = (e * (1.0 / total)).astype(BF16)
                out = jnp.dot(vt[g], probs, preferred_element_type=F32)
                heads[:, cols] = jnp.concatenate([out[:, :ROWS], out[:, ROWS:]], axis=0).T.astype(BF16)

        pieces(PAIRS // PAIR_UNROLL, some_pairs)

    def put_out(number):
        def tile(j):
            cols = rows_at(j * CHUNK, CHUNK, CHUNK)
            parts[number, :, cols] = jnp.dot(
                heads[...], wo[:, cols], preferred_element_type=F32
            ).astype(BF16)

        pieces(D // CHUNK, tile)

    def piece(i, ref, first_row=0):
        return ref.at[pl.ds(first_row + i * SUB, SUB)]

    def small_piece(i, ref, first_row=0):
        row, column, width = TAIL[i]
        return ref.at[pl.ds(first_row + row, SUB), pl.ds(column, width)]

    def send_parts(number, to_left_kind, to_right_kind):
        for i in range(N_P):
            send(
                O_XS,
                XS + jnp.where(to_left_kind == 0, i, 2 * N_P),
                piece(i, parts.at[number]),
                piece(i, xbuf.at[to_left_kind]),
                left,
            )
            send(
                O_XS,
                XS + jnp.where(to_right_kind == 1, N_P + i, 2 * N_P + 1),
                piece(i, parts.at[number], HALF),
                piece(i, xbuf.at[to_right_kind]),
                right,
            )

    kc[...] = jnp.zeros(kc.shape, BF16)
    vs[...] = jnp.zeros(vs.shape, BF16)
    pl.when(jnp.logical_not(yields))(weights_loaded)
    project(own)

    load_mix.wait()
    for copy in load_h:
        copy.wait()
    load_hm.wait()

    def merge(count, dst, theirs, mine_weight, mine):
        def rows(j):
            r = rows_at(j * 16, 16, 16)
            dst[r, :] = (theirs * dst[r, :].astype(F32) + mine_weight * mine[r, :].astype(F32)).astype(BF16)

        pieces(count // 16, rows)

    def far_sum(n):
        i, row, count = FAR[n]
        r = pl.ds(row, count)
        arrived(H13 + n, b13.at[i, r])
        merge(count, b13.at[i, r], weight(3, columns[i], 1), weight(3, columns[i], 0), hl.at[i, r])
        remote(O_H + 1, H03 + n, b13.at[i, r], b03.at[i, r], down).start()

    for k in range(2):
        arrived(AGR + k, quarter(x_left, k))
        to_right(3, x_left, k)
        arrived(AGL + k, quarter(x_right, 2 + k))
        to_left(3, x_right, 2 + k)
        if k == 0:

            @pl.when(y == 0)
            def _():
                far_sum(0)

    @pl.when(x != 0)
    def _():
        to_right(2, x, 2)
        to_right(2, x, 3)

    @pl.when(x == 3)
    def _():
        to_left(2, x, 0)
        to_left(2, x, 1)

    def near_sum(i, h):
        n, rows = 2 * i + h, b02.at[i, kept[h]]
        arrived(H02 + n, rows)
        merge(
            (HALF, KEEP - HALF)[h], rows, weight(2, columns[i], 0), weight(2, columns[i], 1), hl.at[i, kept[h]]
        )
        remote(O_H + 1, H12 + n, rows, b12.at[i, kept[h]], up).start()

    def column_sum(i, row, count, add):
        c = columns[i]

        @pl.when(y == 2)
        def _():
            if row <= HALF:
                h = row // HALF
                arrived(H12 + 2 * i + h, b12.at[i, kept[h]])

                def upper(j):
                    r = rows_at(row + j * 16, 16, 16)
                    add(r, b12[i, r, :].astype(F32))

                pieces((HALF, KEEP - HALF)[h] // 16, upper)
            if row + count == ROWS:
                arrived(H12B + i, b12b.at[i])
                arrived(H02C + i, b02c.at[i])
                one, two = weight(2, c, 1), weight(2, c, 0)

                def lower(j):
                    r = rows_at(j * 16, 16, 16)
                    add(
                        rows_at(KEEP + j * 16, 16, 16),
                        one * b12b[i, r, :].astype(F32) + two * b02c[i, r, :].astype(F32),
                    )

                pieces((ROWS - KEEP) // 16, lower)

        @pl.when(y == 3)
        def _():
            for n, (block, far_row, far_count) in enumerate(FAR):
                if block == i and row <= far_row < row + count:
                    arrived(H03 + n, b03.at[i, pl.ds(far_row, far_count)])
            if row <= HALF:
                h = row // HALF
                arrived(H23 + 2 * i + h, b23.at[i, halves[h]])
            one = weight(3, c, 2)

            def every(j):
                r = rows_at(row + j * 16, 16, 16)
                add(r, b03[i, r, :].astype(F32) + one * b23[i, r, :].astype(F32))

            pieces(count // 16, every)

    nearest_pair = jnp.where(zc == 0, mix[1, jnp.minimum(s + 4, 31)], F32(0.0))

    def for_pair(r, value):
        zs[r, :] = (value + nearest_pair * hm[r, :].astype(F32)).astype(BF16)

    def to_pair(h):
        column_sum(0, h * HALF, HALF, for_pair)

        @pl.when(y >= 2)
        def _():
            remote(O_HZ, HZ + h, zs.at[halves[h]], zr.at[halves[h]], pair).start()

    @pl.when(y == 3)
    def _():
        for i in both:
            arrived(H02B + i, b02b.at[i])
            remote(O_H, H02C + i, b02b.at[i], b02c.at[i], down).start()

    @pl.when(y == 1)
    def _():
        near_sum(0, 0)

    project(first)

    @pl.when(y == 0)
    def _():
        far_sum(1)

    def group_arrived(from_left, from_right):
        arrived(AGR + from_left, xg.at[top])
        arrived(AGL + from_right, xg.at[top])

    @pl.when(y == 1)
    def _():
        near_sum(0, 1)

    left_2 = jnp.where(x == 1, 2, 3)
    right_2 = jnp.where(x == 2, 3, 2)
    group_arrived(left_2, right_2)
    project(second)

    @pl.when(y == 0)
    def _():
        far_sum(2)

    to_pair(0)

    @pl.when(y == 0)
    def _():
        arrived(H01Z, z01)
        for n, (row, count) in enumerate(LAST):
            r = pl.ds(row, count)
            merge(count, z01.at[r], mix[2 + zc - (1 - zc), s + 8], weight(1, zc, 0), hm.at[r])
            remote(O_H + 2, H01 + n, z01.at[r], b01.at[r], up).start()

    load_wo.wait()
    attend(second)
    put_out(2)
    left_kind = jnp.where(x == 1, 2, 0)
    right_kind = jnp.where(x == 2, 1, 3)
    send_parts(2, left_kind, right_kind)

    @pl.when(y == 1)
    def _():
        near_sum(1, 0)

    group_arrived(5 - left_2, 5 - right_2)
    project(third)

    @pl.when(y == 0)
    def _():
        far_sum(3)

    to_pair(1)

    @pl.when(y == 1)
    def _():
        near_sum(1, 1)

    attend(third)
    put_out(3)
    send_parts(3, 2 - left_kind, 4 - right_kind)

    @pl.when(y == 0)
    def _():
        far_sum(4)

    attend(own)

    @pl.when(y == 0)
    def _():
        far_sum(5)

    put_out(0)
    attend(first)
    put_out(1)

    for i in range(N_T):
        row, column, width = TAIL[i]
        cols = pl.ds(column, width)
        for side in both:
            r, rr = pl.ds(row, SUB), pl.ds(side * HALF + row, SUB)
            if column == 0:
                arrived(XS + side * N_P + row // SUB, piece(row // SUB, xbuf.at[side]))
            parts[1, rr, cols] = (
                parts[1, rr, cols].astype(F32) + xbuf[side, r, cols].astype(F32)
            ).astype(BF16)
            send(
                O_XT,
                XT + side * N_T + i,
                small_piece(i, parts.at[1], side * HALF),
                small_piece(i, xtail.at[side]),
                (left, right)[side],
            )

    def with_pair(r, value):
        hs[r, :] = value + zr[r, :].astype(F32)

    @pl.when((y >= 2) | (zc == 1))
    def _():
        for h in both:
            arrived(HZ + h, zr.at[halves[h]])

    nearest = mix[1, s]

    def history_sum(n):
        row, count = LAST[n]
        column_sum(1, row, count, with_pair)

        def every_row(body):
            pieces(count // 16, lambda j: body(rows_at(row + j * 16, 16, 16)))

        @pl.when(y == 0)
        def _():
            def nothing(r):
                hs[r, :] = jnp.zeros((16, D), F32)

            every_row(nothing)

        @pl.when(y == 1)
        def _():
            arrived(H01 + n, b01.at[pl.ds(row, count)])

            def from_row_0(r):
                hs[r, :] = b01[r, :].astype(F32)

            every_row(from_row_0)

        @pl.when((y < 2) & (zc == 1))
        def _():
            def from_pair(r):
                hs[r, :] = hs[r, :] + nearest * zr[r, :].astype(F32)

            every_row(from_pair)

    history_sum(0)
    arrived(XS + 2 * N_P, xbuf.at[2])
    arrived(XS + 2 * N_P + 1, xbuf.at[3])
    own_weight = mix[0, s]
    tail = [(0, 0), (1, 0), 1, (0, 1), (1, 1), (2, 0), (2, 1), 2]
    tail += [(i, side) for i in range(3, N_T) for side in both]
    for step in tail:
        if step in (1, 2):
            history_sum(step)
            continue
        i, side = step
        row, column, width = TAIL[i]
        r, rr = pl.ds(row, SUB), pl.ds(side * HALF + row, SUB)
        arrived(XT + side * N_T + i, small_piece(i, xtail.at[side]))

        def mix_columns(j):
            cols = rows_at(column + j * 1024, 1024, 1024)
            total = (
                parts[0, rr, cols].astype(F32)
                + xtail[side, r, cols].astype(F32)
                + xbuf[3 - side, r, cols].astype(F32)
            )
            block_out = (xv[rr, cols].astype(F32) + total).astype(BF16)
            stage[rr, cols] = (own_weight * block_out.astype(F32) + hs[rr, cols]).astype(BF16)

        pieces(width // 1024, mix_columns)
        send(O_FS, FS, small_piece(i, stage, side * HALF), small_piece(i, out_ref, side * HALF), following)

    def many(rows):
        return xg.at[pl.ds(0, rows)]

    left_here(O_AG, many(3 * ROWS))
    left_here(O_XS, many(2 * ROWS))

    @pl.when(y < 3)
    def _():
        left_here(O_H, many(2 * ROWS))

    @pl.when(y == 3)
    def _():
        left_here(O_H, many(2 * (ROWS - KEEP)))

    @pl.when(y < 2)
    def _():
        left_here(O_H + 1, many(2 * ROWS))

    @pl.when(y == 0)
    def _():
        left_here(O_H + 2, many(2 * ROWS))

    @pl.when((y >= 2) | (zc == 0))
    def _():
        left_here(O_HZ, many(ROWS))

    left_here(O_XT, many(ROWS))
    left_here(O_FS, stage)
    arrived(FS, out_ref)


def on_device(section_input, history, query_weight, key_weight, value_weight, output_weight, mix_weights):
    anywhere = pl.BlockSpec(memory_space=pl.ANY)
    block = (ROWS, D)
    out = pl.pallas_call(
        whole_tick,
        out_shape=pltpu.VMEM(block, BF16),
        in_specs=[anywhere] * 7,
        out_specs=pl.BlockSpec(memory_space=pltpu.VMEM),
        scratch_shapes=[
            pltpu.SMEM((8, 32), F32),
            pltpu.VMEM(block, BF16),
            pltpu.VMEM((SEQ, D), BF16),
            pltpu.VMEM((D, QW + 256), BF16),
            pltpu.VMEM((QW, D), BF16),
            pltpu.VMEM((SEQ, QW + 256), BF16),
            pltpu.VMEM((2, SEQ, 128), BF16),
            pltpu.VMEM((2, HEAD_DIM, SEQ), BF16),
            pltpu.VMEM((SEQ, 128), BF16),
            pltpu.VMEM((ROWS, QW), BF16),
            pltpu.VMEM((4, ROWS, D), BF16),
            pltpu.VMEM((4, HALF, D), BF16),
            pltpu.VMEM((2, HALF, D), BF16),
            pltpu.VMEM((2, KEEP, D), BF16),
            pltpu.VMEM((2, ROWS - KEEP, D), BF16),
            pltpu.VMEM((2, ROWS - KEEP, D), BF16),
            pltpu.VMEM(block, BF16),
            pltpu.VMEM((2, ROWS, D), BF16),
            pltpu.VMEM((2, ROWS, D), BF16),
            pltpu.VMEM((2, ROWS - KEEP, D), BF16),
            pltpu.VMEM((2, KEEP, D), BF16),
            pltpu.VMEM((2, ROWS, D), BF16),
            pltpu.VMEM(block, BF16),
            pltpu.VMEM(block, BF16),
            pltpu.VMEM(block, BF16),
            pltpu.VMEM((2, ROWS, D), BF16),
            pltpu.VMEM(block, BF16),
            pltpu.VMEM(block, F32),
            pltpu.VMEM(block, BF16),
            pltpu.SemaphoreType.DMA((N_LEAVING,)),
            pltpu.SemaphoreType.DMA((N_ARRIVALS,)),
            pltpu.SemaphoreType.DMA((N_LOADS,)),
            pltpu.SemaphoreType.REGULAR,
        ],
        compiler_params=pltpu.CompilerParams(
            collective_id=0, has_side_effects=True, vmem_limit_bytes=60_000_000
        ),
        name="whole_tick",
    )(
        section_input[0], history[0], query_weight[0], key_weight[0], value_weight[0], output_weight[0],
        mix_weights.T,
    )
    return out[None]


def solution(mesh):
    placed = (
        P("section", "tensor", None),
        P("section", None, "tensor", None),
        P("section", None, "tensor"),
        P("section", None, "tensor"),
        P("section", None, "tensor"),
        P("section", "tensor", None),
        P(),
    )
    return jax.shard_map(
        on_device,
        mesh=mesh,
        in_specs=placed,
        out_specs=P("section", "tensor", None),
        check_vma=False,
    )
```

```python
import math

import jax
import jax.numpy as jnp
from jax import lax
from jax.experimental import pallas as pl
from jax.experimental.pallas import tpu as pltpu
from jax.sharding import PartitionSpec as P

HEAD_DIM = 64
MESH = pl.DeviceIdType.MESH
F32 = jnp.float32
BF16 = jnp.bfloat16
ROWS = 128
HALF = 64
D = 4096
SEQ = 512
QW = 768
PAIRS = QW // 128
PAIR_UNROLL = 2
KEEP = 96
QUARTER = 32
FAR = ((0, 0, 32), (0, 32, 32), (0, HALF, HALF), (1, 0, HALF), (1, HALF, 32), (1, 96, 32))
LAST = ((0, HALF), (HALF, 32), (96, 32))
CHUNK = 1024
SUB = 16
LARGE = 32
N_P = HALF // LARGE
TAIL = ((0, 0, D // 2), (0, D // 2, D // 2), (16, 0, D), (32, 0, D), (48, 0, D // 2), (48, D // 2, D // 2))
N_T = len(TAIL)
AGR, AGL = 0, 4
XS = 8
XT = XS + 2 * N_P + 2
FS = XT + 2 * N_T
HZ = FS + 1
H = HZ + 2
H13, H01Z = H, H + 6
H02, H01 = H, H + 4
H12, H12B, H02C = H, H + 4, H + 6
H03, H23, H02B = H, H + 6, H + 10
N_ARRIVALS = H + 12
O_AG, O_XS, O_XT, O_FS, O_HZ, O_H = 0, 1, 2, 3, 4, 5
N_LEAVING = O_H + 3
N_LOADS = 8


def rows_at(start, size, step):
    return pl.ds(pl.multiple_of(start, step), size)


def whole_tick(
    x_hbm, hist_hbm, wq_hbm, wk_hbm, wv_hbm, wo_hbm, mix_hbm, out_ref,
    mix, xv, xg, wqkv, wo, qkv, kc, vt, vs, heads, parts, xbuf, xtail,
    b02, b02b, b02c, b01, b13, b03, b12b, b12, b23, z01, zr, zs, hl, hm, hs, stage,
    send_sem, recv_sem, load_sem, pair_there,
):
    def load(number, src, dst):
        copy = pltpu.make_async_copy(src, dst, load_sem.at[number])
        copy.start()
        return copy

    order = (0, 2, 1, 3)
    load_x = []
    for n, q in enumerate(order):
        r = pl.ds(q * QUARTER, QUARTER)
        load_x.append(load(n, x_hbm.at[r], xv.at[r]))

    s = lax.axis_index("section")
    x = lax.axis_index("tensor")
    core = lax.rem(s, 2)
    y = s // 8
    zc = lax.rem(s // 4, 2)
    x_right, x_left, x_opp = lax.rem(x + 1, 4), lax.rem(x + 3, 4), lax.rem(x + 2, 4)
    right, left = (s, x_right), (s, x_left)
    up, down = (lax.rem(s + 8, 32), x), (lax.rem(s + 24, 32), x)
    pair = (s + 4 - 8 * zc, x)
    following, preceding = (lax.rem(s + 1, 32), x), (lax.rem(s + 31, 32), x)

    barrier = pltpu.get_barrier_semaphore()
    for other in (right, left, up, down, preceding):
        pl.semaphore_signal(barrier, inc=1, device_id=other, device_id_type=MESH)

    @pl.when(zc == 0)
    def _():
        pl.semaphore_signal(barrier, inc=1, device_id=pair, device_id_type=MESH)

    def remote(leaving, number, src, dst, device):
        return pltpu.make_async_remote_copy(
            src_ref=src,
            dst_ref=dst,
            send_sem=send_sem.at[leaving],
            recv_sem=recv_sem.at[number],
            device_id=device,
            device_id_type=MESH,
        )

    def send(leaving, number, src, dst, device):
        remote(leaving, number, src, dst, device).start()

    def arrived(number, ref):
        remote(0, number, ref, ref, pair).wait_recv()

    def left_here(leaving, ref):
        remote(leaving, 0, ref, ref, pair).wait_send()

    def pieces(count, body):
        def step(j, carry):
            body(j)
            return carry

        lax.fori_loop(0, count, step, 0)

    columns = (1 - zc, zc)
    both = (0, 1)
    top, bottom = pl.ds(0, HALF), pl.ds(HALF, HALF)
    halves = (top, bottom)
    rest = pl.ds(KEEP, ROWS - KEEP)
    kept = (top, pl.ds(HALF, KEEP - HALF))

    def slot(dy, i):
        return 2 * dy + columns[i] - zc - 1

    def quarter(block, q):
        return xg.at[rows_at(block * ROWS + q * QUARTER, QUARTER, QUARTER)]

    def to_right(number, block, q):
        send(O_AG, AGR + number, quarter(block, q), quarter(block, q), right)

    def to_left(number, block, q):
        send(O_AG, AGL + number, quarter(block, q), quarter(block, q), left)

    own = (x * ROWS, x * ROWS + HALF)
    first = (x_left * ROWS, x_right * ROWS + HALF)
    second = (
        jnp.where(x == 1, x_left * ROWS + HALF, x_opp * ROWS),
        jnp.where(x == 2, x_opp * ROWS + HALF, x_right * ROWS),
    )
    third = (
        jnp.where(x == 1, x_opp * ROWS, x_left * ROWS + HALF),
        jnp.where(x == 2, x_right * ROWS, x_opp * ROWS + HALF),
    )

    for n, q in enumerate(order):
        load_x[n].wait()

        def normalize_rows(j):
            r = rows_at(q * QUARTER + j * 16, 16, 16)
            values = xv[r, :].astype(F32)
            inv = lax.rsqrt(jnp.mean(values * values, axis=-1, keepdims=True) + 1e-05)
            xg[rows_at(x * ROWS + q * QUARTER + j * 16, 16, 16), :] = (values * inv).astype(BF16)

        if n < 2:
            for j in range(QUARTER // 16):
                normalize_rows(j)
                if n == 0 and j == 0:
                    pl.semaphore_wait(barrier, 5 + zc)

                    @pl.when(zc == 1)
                    def _():
                        pl.semaphore_signal(pair_there, inc=1, device_id=pair, device_id_type=MESH)

                def out_rows():
                    rows = xg.at[rows_at(x * ROWS + q * QUARTER + j * 16, 16, 16)]
                    send(O_AG, (AGR, AGL)[n], rows, rows, (right, left)[n])

                pl.when(core == 1)(out_rows)
            continue

        pieces(QUARTER // 16, normalize_rows)

        def out_quarter():
            if q < 2:
                to_right(q, x, q)
            else:
                to_left(q - 2, x, q)

        pl.when(core == 1)(out_quarter)

    def stored_history():
        @pl.when(y == 0)
        def _():
            for i in both:
                for h in both:
                    remote(O_H, H02 + 2 * i + h, hist_hbm.at[slot(2, i), kept[h]], b02.at[i, kept[h]], up).start()
                remote(O_H, H02B + i, hist_hbm.at[slot(2, i), rest], b02b.at[i], down).start()

        @pl.when(y == 1)
        def _():
            for n, (i, row, count) in enumerate(FAR):
                r = pl.ds(row, count)
                remote(O_H, H13 + n, hist_hbm.at[slot(2, i), r], b13.at[i, r], down).start()
            for i in both:
                remote(O_H + 1, H12B + i, hist_hbm.at[slot(1, i), rest], b12b.at[i], up).start()

        @pl.when(y == 2)
        def _():
            for i in both:
                for h in both:
                    remote(O_H, H23 + 2 * i + h, hist_hbm.at[slot(1, i), halves[h]], b23.at[i, halves[h]], up).start()

    pl.when(core == 1)(stored_history)

    load_kv = [
        load(5, wk_hbm, wqkv.at[:, pl.ds(QW, 128)]),
        load(6, wv_hbm, wqkv.at[:, pl.ds(QW + 128, 128)]),
    ]
    load_q = load(4, wq_hbm, wqkv.at[:, pl.ds(0, QW)])
    load_mix = load(7, mix_hbm, mix)
    far = jnp.where(y == 0, 3, 1)
    load_h = [load(i, hist_hbm.at[slot(far, i)], hl.at[i]) for i in both]
    load_hm = load(2, hist_hbm.at[jnp.where(y == 0, 1, 0)], hm)
    load_wo = load(3, wo_hbm, wo)

    yields = (core == 0) & (lax.rem(s // 2, 4) == 3)

    def weights_loaded():
        for copy in load_kv:
            copy.wait()
        load_q.wait()

    pl.when(yields)(weights_loaded)

    @pl.when(core == 0)
    def _():
        stored_history()
        to_right(0, x, 0)
        to_left(0, x, 2)
        to_right(1, x, 1)
        to_left(1, x, 3)

    @pl.when(x == 0)
    def _():
        to_right(2, x, 2)
        to_right(2, x, 3)

    @pl.when(x != 3)
    def _():
        to_left(2, x, 0)
        to_left(2, x, 1)

    @pl.when(zc == 0)
    def _():
        pl.semaphore_wait(pair_there, 1)

    @pl.when(y == 0)
    def _():
        remote(O_H + 2, H01Z, hist_hbm.at[slot(1, 0)], z01, pair).start()

    @pl.when((y < 2) & (zc == 0))
    def _():
        for h in both:
            remote(O_HZ, HZ + h, hist_hbm.at[0, halves[h]], zr.at[halves[h]], pair).start()

    def weight(y_dst, c, y_src):
        return mix[2 * (y_dst - y_src) + c - zc, y_dst * 8 + c * 4 + lax.rem(s, 4)]

    def project(group):
        r0, r1 = (rows_at(start, HALF, HALF) for start in group)

        def tile(j):
            cols = rows_at(j * 256, 256, 256)
            tokens = jnp.concatenate([xg[r0, :], xg[r1, :]], axis=0)
            out = jnp.dot(tokens, wqkv[:, cols], preferred_element_type=F32).astype(BF16)
            qkv[r0, cols] = out[:HALF]
            qkv[r1, cols] = out[HALF:]

        pieces(4, tile)
        low = lax.broadcasted_iota(jnp.int32, (HALF, 128), 1) < HEAD_DIM
        for r in (r0, r1):
            keys = qkv[r, pl.ds(QW, 128)].astype(F32)
            turned = pltpu.roll(keys, HEAD_DIM, 1)
            kc[0, r, :] = jnp.where(low, keys, turned).astype(BF16)
            kc[1, r, :] = jnp.where(low, turned, keys).astype(BF16)
            vs[r, :] = qkv[r, pl.ds(QW + 128, 128)]

    exponent_scale = math.log2(math.e) / math.sqrt(HEAD_DIM)

    def attend(group):
        r0, r1 = (rows_at(start, HALF, HALF) for start in group)
        lane = lax.broadcasted_iota(jnp.int32, (SEQ, 2 * ROWS), 1)
        lane = jnp.where(lane < ROWS, lane, lane - ROWS)
        query = lane + jnp.where(lane < HALF, group[0], group[1] - HALF)
        seen = query >= lax.broadcasted_iota(jnp.int32, (SEQ, 2 * ROWS), 0)
        low = lax.broadcasted_iota(jnp.int32, (ROWS, 128), 1) < HEAD_DIM
        turned_values = vs[...].astype(F32).T.astype(BF16)
        vt[0] = turned_values[:HEAD_DIM]
        vt[1] = turned_values[HEAD_DIM:]

        def some_pairs(j):
            for k in range(PAIR_UNROLL):
                p = PAIR_UNROLL * j + k
                g = p // (PAIRS // 2)
                cols = rows_at(p * 128, 128, 128)
                q = jnp.concatenate([qkv[r0, cols], qkv[r1, cols]], axis=0)
                zero = jnp.zeros_like(q)
                apart = jnp.concatenate([jnp.where(low, q, zero), jnp.where(low, zero, q)], axis=0)
                scores = lax.dot_general(kc[g], apart, (((1,), (1,)), ((), ())), preferred_element_type=F32)
                scores = jnp.where(seen, scores, -1e30)
                high = jnp.max(scores, axis=0, keepdims=True)
                e = jnp.exp2((scores - high) * exponent_scale)
                total = jnp.sum(e, axis=0, keepdims=True)
                probs = (e * (1.0 / total)).astype(BF16)
                out = jnp.dot(vt[g], probs, preferred_element_type=F32)
                heads[:, cols] = jnp.concatenate([out[:, :ROWS], out[:, ROWS:]], axis=0).T.astype(BF16)

        pieces(PAIRS // PAIR_UNROLL, some_pairs)

    def put_out(number):
        def tile(j):
            cols = rows_at(j * CHUNK, CHUNK, CHUNK)
            parts[number, :, cols] = jnp.dot(
                heads[...], wo[:, cols], preferred_element_type=F32
            ).astype(BF16)

        pieces(D // CHUNK, tile)

    def piece(i, ref, first_row=0):
        return ref.at[pl.ds(first_row + i * LARGE, LARGE)]

    def small_piece(i, ref, first_row=0):
        row, column, width = TAIL[i]
        return ref.at[pl.ds(first_row + row, SUB), pl.ds(column, width)]

    def send_parts(number, to_left_kind, to_right_kind):
        for i in range(N_P):
            send(
                O_XS,
                XS + jnp.where(to_left_kind == 0, i, 2 * N_P),
                piece(i, parts.at[number]),
                piece(i, xbuf.at[to_left_kind]),
                left,
            )
            send(
                O_XS,
                XS + jnp.where(to_right_kind == 1, N_P + i, 2 * N_P + 1),
                piece(i, parts.at[number], HALF),
                piece(i, xbuf.at[to_right_kind]),
                right,
            )

    kc[...] = jnp.zeros(kc.shape, BF16)
    vs[...] = jnp.zeros(vs.shape, BF16)
    pl.when(jnp.logical_not(yields))(weights_loaded)
    project(own)

    load_mix.wait()
    for copy in load_h:
        copy.wait()
    load_hm.wait()

    def merge(count, dst, theirs, mine_weight, mine):
        def rows(j):
            r = rows_at(j * 16, 16, 16)
            dst[r, :] = (theirs * dst[r, :].astype(F32) + mine_weight * mine[r, :].astype(F32)).astype(BF16)

        pieces(count // 16, rows)

    def far_sum(n):
        i, row, count = FAR[n]
        r = pl.ds(row, count)
        arrived(H13 + n, b13.at[i, r])
        merge(count, b13.at[i, r], weight(3, columns[i], 1), weight(3, columns[i], 0), hl.at[i, r])
        remote(O_H + 1, H03 + n, b13.at[i, r], b03.at[i, r], down).start()

    for k in range(2):
        arrived(AGR + k, quarter(x_left, k))
        to_right(3, x_left, k)
        arrived(AGL + k, quarter(x_right, 2 + k))
        to_left(3, x_right, 2 + k)
        if k == 0:

            @pl.when(y == 0)
            def _():
                far_sum(0)

    @pl.when(x != 0)
    def _():
        to_right(2, x, 2)
        to_right(2, x, 3)

    @pl.when(x == 3)
    def _():
        to_left(2, x, 0)
        to_left(2, x, 1)

    def near_sum(i, h):
        n, rows = 2 * i + h, b02.at[i, kept[h]]
        arrived(H02 + n, rows)
        merge(
            (HALF, KEEP - HALF)[h], rows, weight(2, columns[i], 0), weight(2, columns[i], 1), hl.at[i, kept[h]]
        )
        remote(O_H + 1, H12 + n, rows, b12.at[i, kept[h]], up).start()

    def column_sum(i, row, count, add):
        c = columns[i]

        @pl.when(y == 2)
        def _():
            if row <= HALF:
                h = row // HALF
                arrived(H12 + 2 * i + h, b12.at[i, kept[h]])

                def upper(j):
                    r = rows_at(row + j * 16, 16, 16)
                    add(r, b12[i, r, :].astype(F32))

                pieces((HALF, KEEP - HALF)[h] // 16, upper)
            if row + count == ROWS:
                arrived(H12B + i, b12b.at[i])
                arrived(H02C + i, b02c.at[i])
                one, two = weight(2, c, 1), weight(2, c, 0)

                def lower(j):
                    r = rows_at(j * 16, 16, 16)
                    add(
                        rows_at(KEEP + j * 16, 16, 16),
                        one * b12b[i, r, :].astype(F32) + two * b02c[i, r, :].astype(F32),
                    )

                pieces((ROWS - KEEP) // 16, lower)

        @pl.when(y == 3)
        def _():
            for n, (block, far_row, far_count) in enumerate(FAR):
                if block == i and row <= far_row < row + count:
                    arrived(H03 + n, b03.at[i, pl.ds(far_row, far_count)])
            if row <= HALF:
                h = row // HALF
                arrived(H23 + 2 * i + h, b23.at[i, halves[h]])
            one = weight(3, c, 2)

            def every(j):
                r = rows_at(row + j * 16, 16, 16)
                add(r, b03[i, r, :].astype(F32) + one * b23[i, r, :].astype(F32))

            pieces(count // 16, every)

    nearest_pair = jnp.where(zc == 0, mix[1, jnp.minimum(s + 4, 31)], F32(0.0))

    def for_pair(r, value):
        zs[r, :] = (value + nearest_pair * hm[r, :].astype(F32)).astype(BF16)

    def to_pair(h):
        column_sum(0, h * HALF, HALF, for_pair)

        @pl.when(y >= 2)
        def _():
            remote(O_HZ, HZ + h, zs.at[halves[h]], zr.at[halves[h]], pair).start()

    @pl.when(y == 3)
    def _():
        for i in both:
            arrived(H02B + i, b02b.at[i])
            remote(O_H, H02C + i, b02b.at[i], b02c.at[i], down).start()

    @pl.when(y == 1)
    def _():
        near_sum(0, 0)

    project(first)

    @pl.when(y == 0)
    def _():
        far_sum(1)

    def group_arrived(from_left, from_right):
        arrived(AGR + from_left, xg.at[top])
        arrived(AGL + from_right, xg.at[top])

    @pl.when(y == 1)
    def _():
        near_sum(0, 1)

    left_2 = jnp.where(x == 1, 2, 3)
    right_2 = jnp.where(x == 2, 3, 2)
    group_arrived(left_2, right_2)
    project(second)

    @pl.when(y == 0)
    def _():
        far_sum(2)

    to_pair(0)

    @pl.when(y == 0)
    def _():
        arrived(H01Z, z01)
        for n, (row, count) in enumerate(LAST):
            r = pl.ds(row, count)
            merge(count, z01.at[r], mix[2 + zc - (1 - zc), s + 8], weight(1, zc, 0), hm.at[r])
            remote(O_H + 2, H01 + n, z01.at[r], b01.at[r], up).start()

    load_wo.wait()
    attend(second)
    put_out(2)
    left_kind = jnp.where(x == 1, 2, 0)
    right_kind = jnp.where(x == 2, 1, 3)
    send_parts(2, left_kind, right_kind)

    @pl.when(y == 1)
    def _():
        near_sum(1, 0)

    group_arrived(5 - left_2, 5 - right_2)
    project(third)

    @pl.when(y == 0)
    def _():
        far_sum(3)

    to_pair(1)

    @pl.when(y == 1)
    def _():
        near_sum(1, 1)

    attend(third)
    put_out(3)
    send_parts(3, 2 - left_kind, 4 - right_kind)

    @pl.when(y == 0)
    def _():
        far_sum(4)

    attend(own)

    @pl.when(y == 0)
    def _():
        far_sum(5)

    put_out(0)
    attend(first)
    put_out(1)

    for i in range(N_T):
        row, column, width = TAIL[i]
        cols = pl.ds(column, width)
        for side in both:
            r, rr = pl.ds(row, SUB), pl.ds(side * HALF + row, SUB)
            if column == 0 and row % LARGE == 0:
                arrived(XS + side * N_P + row // LARGE, piece(row // LARGE, xbuf.at[side]))
            parts[1, rr, cols] = (
                parts[1, rr, cols].astype(F32) + xbuf[side, r, cols].astype(F32)
            ).astype(BF16)
            send(
                O_XT,
                XT + side * N_T + i,
                small_piece(i, parts.at[1], side * HALF),
                small_piece(i, xtail.at[side]),
                (left, right)[side],
            )

    def with_pair(r, value):
        hs[r, :] = value + zr[r, :].astype(F32)

    @pl.when((y >= 2) | (zc == 1))
    def _():
        for h in both:
            arrived(HZ + h, zr.at[halves[h]])

    nearest = mix[1, s]

    def history_sum(n):
        row, count = LAST[n]
        column_sum(1, row, count, with_pair)

        def every_row(body):
            pieces(count // 16, lambda j: body(rows_at(row + j * 16, 16, 16)))

        @pl.when(y == 0)
        def _():
            def nothing(r):
                hs[r, :] = jnp.zeros((16, D), F32)

            every_row(nothing)

        @pl.when(y == 1)
        def _():
            arrived(H01 + n, b01.at[pl.ds(row, count)])

            def from_row_0(r):
                hs[r, :] = b01[r, :].astype(F32)

            every_row(from_row_0)

        @pl.when((y < 2) & (zc == 1))
        def _():
            def from_pair(r):
                hs[r, :] = hs[r, :] + nearest * zr[r, :].astype(F32)

            every_row(from_pair)

    history_sum(0)
    arrived(XS + 2 * N_P, xbuf.at[2])
    arrived(XS + 2 * N_P + 1, xbuf.at[3])
    own_weight = mix[0, s]
    tail = [(0, 0), (1, 0), 1, (0, 1), (1, 1), (2, 0), (2, 1), 2]
    tail += [(i, side) for i in range(3, N_T) for side in both]
    for step in tail:
        if step in (1, 2):
            history_sum(step)
            continue
        i, side = step
        row, column, width = TAIL[i]
        r, rr = pl.ds(row, SUB), pl.ds(side * HALF + row, SUB)
        arrived(XT + side * N_T + i, small_piece(i, xtail.at[side]))

        def mix_columns(j):
            cols = rows_at(column + j * 1024, 1024, 1024)
            total = (
                parts[0, rr, cols].astype(F32)
                + xtail[side, r, cols].astype(F32)
                + xbuf[3 - side, r, cols].astype(F32)
            )
            block_out = (xv[rr, cols].astype(F32) + total).astype(BF16)
            stage[rr, cols] = (own_weight * block_out.astype(F32) + hs[rr, cols]).astype(BF16)

        pieces(width // 1024, mix_columns)
        send(O_FS, FS, small_piece(i, stage, side * HALF), small_piece(i, out_ref, side * HALF), following)

    def many(rows):
        return xg.at[pl.ds(0, rows)]

    left_here(O_AG, many(3 * ROWS))
    left_here(O_XS, many(2 * ROWS))

    @pl.when(y < 3)
    def _():
        left_here(O_H, many(2 * ROWS))

    @pl.when(y == 3)
    def _():
        left_here(O_H, many(2 * (ROWS - KEEP)))

    @pl.when(y < 2)
    def _():
        left_here(O_H + 1, many(2 * ROWS))

    @pl.when(y == 0)
    def _():
        left_here(O_H + 2, many(2 * ROWS))

    @pl.when((y >= 2) | (zc == 0))
    def _():
        left_here(O_HZ, many(ROWS))

    left_here(O_XT, many(ROWS))
    left_here(O_FS, stage)
    arrived(FS, out_ref)


def on_device(section_input, history, query_weight, key_weight, value_weight, output_weight, mix_weights):
    anywhere = pl.BlockSpec(memory_space=pl.ANY)
    block = (ROWS, D)
    out = pl.pallas_call(
        whole_tick,
        out_shape=pltpu.VMEM(block, BF16),
        in_specs=[anywhere] * 7,
        out_specs=pl.BlockSpec(memory_space=pltpu.VMEM),
        scratch_shapes=[
            pltpu.SMEM((8, 32), F32),
            pltpu.VMEM(block, BF16),
            pltpu.VMEM((SEQ, D), BF16),
            pltpu.VMEM((D, QW + 256), BF16),
            pltpu.VMEM((QW, D), BF16),
            pltpu.VMEM((SEQ, QW + 256), BF16),
            pltpu.VMEM((2, SEQ, 128), BF16),
            pltpu.VMEM((2, HEAD_DIM, SEQ), BF16),
            pltpu.VMEM((SEQ, 128), BF16),
            pltpu.VMEM((ROWS, QW), BF16),
            pltpu.VMEM((4, ROWS, D), BF16),
            pltpu.VMEM((4, HALF, D), BF16),
            pltpu.VMEM((2, HALF, D), BF16),
            pltpu.VMEM((2, KEEP, D), BF16),
            pltpu.VMEM((2, ROWS - KEEP, D), BF16),
            pltpu.VMEM((2, ROWS - KEEP, D), BF16),
            pltpu.VMEM(block, BF16),
            pltpu.VMEM((2, ROWS, D), BF16),
            pltpu.VMEM((2, ROWS, D), BF16),
            pltpu.VMEM((2, ROWS - KEEP, D), BF16),
            pltpu.VMEM((2, KEEP, D), BF16),
            pltpu.VMEM((2, ROWS, D), BF16),
            pltpu.VMEM(block, BF16),
            pltpu.VMEM(block, BF16),
            pltpu.VMEM(block, BF16),
            pltpu.VMEM((2, ROWS, D), BF16),
            pltpu.VMEM(block, BF16),
            pltpu.VMEM(block, F32),
            pltpu.VMEM(block, BF16),
            pltpu.SemaphoreType.DMA((N_LEAVING,)),
            pltpu.SemaphoreType.DMA((N_ARRIVALS,)),
            pltpu.SemaphoreType.DMA((N_LOADS,)),
            pltpu.SemaphoreType.REGULAR,
        ],
        compiler_params=pltpu.CompilerParams(
            collective_id=0, has_side_effects=True, vmem_limit_bytes=60_000_000
        ),
        name="whole_tick",
    )(
        section_input[0], history[0], query_weight[0], key_weight[0], value_weight[0], output_weight[0],
        mix_weights.T,
    )
    return out[None]


def solution(mesh):
    placed = (
        P("section", "tensor", None),
        P("section", None, "tensor", None),
        P("section", None, "tensor"),
        P("section", None, "tensor"),
        P("section", None, "tensor"),
        P("section", "tensor", None),
        P(),
    )
    return jax.shard_map(
        on_device,
        mesh=mesh,
        in_specs=placed,
        out_specs=P("section", "tensor", None),
        check_vma=False,
    )
```
